256 devices in a mesh: blk: 128 (over y_hi, x, z, core), grp: 2 (over y_lo).
Axes of the slice: x: 4, y: 4 (y_hi: 2, y_lo: 2; y = y_hi * 2 + y_lo), z: 8, core: 2. Of those that a mesh axis runs over, the one named last changes fastest.
Arguments:
- embeddings: bfloat16 [262144, 1024], P(('blk', 'grp')), may hold values from -6 to 6
Outputs:
- tile_max: float32 [262144, 40], P(('blk', 'grp'))
The draws below stay inside these ranges and needn't reach their ends.
All inputs are finite; a program needn't handle non-finite values.
Results may differ from the reference program's by a relative error of at most 0.0017.
Values may be sent and summed in bfloat16 or wider, within the bound.
A program may use at most 64 MiB of HBM per device.

```python
import jax
import jax.numpy as jnp
from jax import lax

D = 1024
R_DEV = 1024
TILES = 8
BLOCKS = 256
ROWS = 262144


def steps_of(key, extent, split, least, largest):
    loudness = 1.0
    for axis_at, shards_of in split:
        heights = jax.random.uniform(jax.random.fold_in(jax.random.fold_in(key, 6), axis_at), (shards_of,), jnp.float32, least / len(split), largest / len(split))
        loudness = loudness * jnp.repeat(jnp.exp(heights), extent[axis_at] // shards_of).reshape((-1,) + (1,) * (len(extent) - 1 - axis_at))
    return loudness


def normal_values(own_key, dims, deviation, most, split=(), held_as=jnp.bfloat16):
    array = jax.random.normal(own_key, dims, jnp.float32) * deviation
    if len(split) > 0:
        array = steps_of(own_key, dims, split, -0.22, 0.18) * array
    return jnp.clip(array, min=-most, max=most).astype(held_as)


def setup_inputs(seed: int = 0) -> dict:
    splits = jax.random.split(jax.random.key(seed), 2)
    return {
        "embeddings": normal_values(splits[0], (ROWS, D), 1.0, 6.0, ((0, 256),)),
    }


def tile_rows(scores):
    count = scores.shape[0]
    return lax.optimization_barrier(jnp.max(scores.reshape(count, count // 128, 128), axis=-1))

def tile_columns(scores):
    count = scores.shape[0]
    return jnp.transpose(lax.optimization_barrier(jnp.max(scores.reshape(count // 128, 128, count), axis=1)))

def reference(embeddings):
    values = embeddings.astype(jnp.float32)
    unit = (values * lax.rsqrt(lax.optimization_barrier(jnp.mean(values * values, axis=-1, keepdims=True)) + 1e-06)).astype(jnp.bfloat16)
    blocks = unit.reshape(BLOCKS, R_DEV, D)
    next_one = jnp.roll(blocks, -1, axis=0)
    next_two = jnp.roll(blocks, -2, axis=0)
    scale = 1.0 / D ** 0.5
    same = jnp.arange(R_DEV)[:, None] == jnp.arange(R_DEV)[None, :]

    def score(queries, keys):
        return lax.dot_general(queries, keys, (((1,), (1,)), ((), ())), preferred_element_type=jnp.float32) * scale

    def per_block(triple):
        queries, first, second = triple
        own = jnp.where(same, -jnp.inf, score(queries, queries))
        one = score(queries, first)
        two = score(queries, second)
        return (tile_rows(own), tile_rows(one), tile_rows(two), tile_columns(one), tile_columns(two))
    own_max, one_max, two_max, col_one, col_two = lax.map(per_block, (blocks, next_one, next_two))
    back_one = jnp.roll(col_one, 1, axis=0)
    back_two = jnp.roll(col_two, 2, axis=0)
    joined = jnp.concatenate([back_two, back_one, own_max, one_max, two_max], axis=2)
    return joined.reshape(ROWS, 5 * TILES)
```

```python
import functools

import jax
import jax.numpy as jnp
from jax import lax
from jax.experimental import pallas as pl
from jax.experimental.pallas import tpu as pltpu
from jax.sharding import PartitionSpec as P

MESH = pl.DeviceIdType.MESH
ROWS = 1024
TILE = 128
TILES = ROWS // TILE
GRP = 2
BLOCKS = 256


def where_of(block):
    block = lax.rem(block + BLOCKS, BLOCKS)
    return (lax.div(block, GRP), lax.rem(block, GRP))


def unit_rows(raw):
    values = raw.astype(jnp.float32)
    return (values * lax.rsqrt(jnp.mean(values * values, axis=-1, keepdims=True) + 1e-06)).astype(
        jnp.bfloat16
    )


def kernel(
    x_ref,
    out_ref,
    raw,
    unit,
    near,
    far,
    extra,
    back,
    load_sem,
    send_sem,
    near_sem,
    far_sem,
    extra_sem,
    back_send_sem,
    back_sem,
):
    b = lax.axis_index("blk") * GRP + lax.axis_index("grp")
    m = lax.rem(b, 4)
    z = lax.rem(lax.div(b, 4), 8)
    x = lax.rem(lax.div(b, 32), 4)
    scale = 1.0 / 1024**0.5

    is_e = x >= 2
    s = jnp.where(is_e, -1, 1)
    role = jnp.where(is_e, 3 - m, m)
    even = lax.rem(role, 2) == 0
    odd = jnp.logical_not(even)
    first_o = jnp.logical_and(x == 0, z == 0)
    first_e = jnp.logical_and(x == 2, z == 0)
    last_e = jnp.logical_and(x == 3, z == 7)
    low = m < 2

    mate = b + 1 - 2 * lax.rem(m, 2)
    no_far = jnp.logical_and(first_e, low)
    has_far = jnp.logical_not(no_far)
    no_send = jnp.logical_or(
        jnp.logical_and(first_o, low), jnp.logical_and(last_e, jnp.logical_not(low))
    )
    sends_far = jnp.logical_not(no_send)
    cross_e = jnp.logical_and(last_e, m == 3)
    cross_o = jnp.logical_and(first_o, m == 0)
    cross = jnp.logical_or(cross_e, cross_o)
    over = jnp.where(is_e, b + 1, b - 1)

    load = pltpu.make_async_copy(x_ref, raw, load_sem)
    load.start()

    barrier = pltpu.get_barrier_semaphore()

    def greet(block):
        pl.semaphore_signal(barrier, inc=1, device_id=where_of(block), device_id_type=MESH)

    greet(mate)
    greet(b + 2 * s)

    @pl.when(sends_far)
    def _():
        greet(b - 2 * s)

    @pl.when(cross)
    def _():
        greet(over)

    count = 2 + sends_far.astype(jnp.int32) + cross.astype(jnp.int32)
    pl.semaphore_wait(barrier, count)
    load.wait()

    def block_copy(dst, sems, which, t, block):
        rows = pl.ds(pl.multiple_of(t * TILE, TILE), TILE)
        return pltpu.make_async_remote_copy(
            src_ref=raw.at[rows],
            dst_ref=dst.at[rows],
            send_sem=send_sem.at[which, t],
            recv_sem=sems.at[t],
            device_id=where_of(block),
            device_id_type=MESH,
        )

    def each_tile(body):
        def step(t, carry):
            body(t)
            return carry

        lax.fori_loop(0, TILES, step, 0)

    def send_all(cond, dst, sems, which, block):
        @pl.when(cond)
        def _():
            each_tile(lambda t: block_copy(dst, sems, which, t, block).start())

    def settle(cond, dst, sems, which, block):
        @pl.when(cond)
        def _():
            each_tile(lambda t: block_copy(dst, sems, which, t, block).wait_send())

    sends = [
        (odd, near, near_sem, 0, mate),
        (sends_far, far, far_sem, 1, b - 2 * s),
        (no_far, far, far_sem, 2, b + 2 * s),
        (cross, extra, extra_sem, 3, over),
    ]
    for send in sends:
        send_all(*send)

    def make_unit(t):
        rows = pl.ds(pl.multiple_of(t * TILE, TILE), TILE)
        unit[rows, :] = unit_rows(raw[rows, :])

    each_tile(make_unit)

    def scores(left, right):
        return lax.dot_general(
            left, right, (((1,), (1,)), ((), ())), preferred_element_type=jnp.float32
        )

    def own_tile(t):
        rows = pl.ds(pl.multiple_of(t * TILE, TILE), TILE)
        left = unit[rows, :]
        for n in range(4):
            block = scores(left, unit[n * 256 : n * 256 + 256, :])
            at = lax.broadcasted_iota(jnp.int32, (TILE, 256), 0) + t * TILE
            to = lax.broadcasted_iota(jnp.int32, (TILE, 256), 1) + n * 256
            block = jnp.where(at == to, -jnp.inf, block)
            out_ref[pl.ds(16 + t, 1), n * 256 : n * 256 + 256] = (
                jnp.max(block, axis=0, keepdims=True) * scale
            )

    each_tile(own_tile)

    def pair_tile(left, rows_ref, t, by_row, row_base, by_key, key_base):
        columns = pl.ds(pl.multiple_of(t * TILE, TILE), TILE)
        for n in range(4):
            block = scores(left, rows_ref[n * 256 : n * 256 + 256, :])
            by_row[pl.ds(row_base + t, 1), n * 256 : n * 256 + 256] = (
                jnp.max(block, axis=0, keepdims=True) * scale
            )
            for h in range(2):
                turned = jnp.transpose(block[:, h * 128 : h * 128 + 128])
                by_key[pl.ds(key_base + 2 * n + h, 1), columns] = (
                    jnp.max(turned, axis=0, keepdims=True) * scale
                )

    def slot(offset):
        return pl.multiple_of((offset + 2) * TILES, TILES)

    def arrive(t, ref, sems):
        rows = pl.ds(pl.multiple_of(t * TILE, TILE), TILE)
        pltpu.make_async_copy(raw.at[rows], ref.at[rows], sems.at[t]).wait()
        left = unit_rows(ref[rows, :])
        ref[rows, :] = left
        return left

    def message(k, block, offset):
        return pltpu.make_async_remote_copy(
            src_ref=back.at[pl.ds(k * TILES, TILES)],
            dst_ref=out_ref.at[pl.ds(slot(offset), TILES)],
            send_sem=back_send_sem.at[k],
            recv_sem=back_sem.at[offset + 2],
            device_id=where_of(block),
            device_id_type=MESH,
        )

    @pl.when(has_far)
    def _():
        each_tile(
            lambda t: pair_tile(
                arrive(t, far, far_sem), unit, t, out_ref, slot(2 * s), back, 0
            )
        )
        message(0, b + 2 * s, -2 * s).start()

    @pl.when(even)
    def _():
        def near_tile(t):
            left = arrive(t, near, near_sem)
            pair_tile(left, unit, t, out_ref, slot(s), back, TILES)

            @pl.when(has_far)
            def _():
                pair_tile(left, far, t, back, 2 * TILES, back, 3 * TILES)

        each_tile(near_tile)
        message(1, mate, -s).start()

        @pl.when(has_far)
        def _():
            message(2, b + 2 * s, -s).start()
            message(3, mate, s).start()

    @pl.when(cross_e)
    def _():
        def seam_tile(t):
            left = arrive(t, extra, extra_sem)
            pair_tile(left, unit, t, out_ref, slot(1), back, 4 * TILES)
            pair_tile(left, near, t, back, 5 * TILES, back, 6 * TILES)

        each_tile(seam_tile)
        message(4, over, -1).start()
        message(5, mate, 2).start()
        message(6, over, -2).start()

    @pl.when(cross_o)
    def _():
        def seam_tile(t):
            left = arrive(t, extra, extra_sem)
            pair_tile(left, near, t, back, 5 * TILES, back, 6 * TILES)

        each_tile(seam_tile)
        message(5, mate, -2).start()
        message(6, over, 2).start()

    def landed(offset):
        rows = pl.ds(slot(offset), TILES)
        pltpu.make_async_copy(
            back.at[pl.ds(0, TILES)], out_ref.at[rows], back_sem.at[offset + 2]
        ).wait()

    landed(-2 * s)

    @pl.when(jnp.logical_not(cross_e))
    def _():
        landed(-s)

    @pl.when(odd)
    def _():
        @pl.when(has_far)
        def _():
            landed(s)

    @pl.when(no_far)
    def _():
        landed(2 * s)

        @pl.when(odd)
        def _():
            landed(s)

    for send in sends:
        settle(*send)

    @pl.when(has_far)
    def _():
        message(0, b + 2 * s, -2 * s).wait_send()

    @pl.when(even)
    def _():
        message(1, mate, -s).wait_send()

        @pl.when(has_far)
        def _():
            message(2, b + 2 * s, -s).wait_send()
            message(3, mate, s).wait_send()

    @pl.when(cross_e)
    def _():
        message(4, over, -1).wait_send()

    @pl.when(cross)
    def _():
        message(5, mate, 2 * s).wait_send()
        message(6, over, 2 * s).wait_send()


def body(embeddings):
    rows, width = embeddings.shape
    block = pltpu.VMEM((rows, width), jnp.bfloat16)
    tiles_t = pl.pallas_call(
        kernel,
        name="cycle_tile_max",
        out_shape=jax.ShapeDtypeStruct((5 * TILES, rows), jnp.float32),
        in_specs=[pl.BlockSpec(memory_space=pltpu.HBM)],
        out_specs=pl.BlockSpec(memory_space=pltpu.VMEM),
        scratch_shapes=[
            block,
            block,
            block,
            block,
            block,
            pltpu.VMEM((7 * TILES, rows), jnp.float32),
            pltpu.SemaphoreType.DMA,
            pltpu.SemaphoreType.DMA((4, TILES)),
            pltpu.SemaphoreType.DMA((TILES,)),
            pltpu.SemaphoreType.DMA((TILES,)),
            pltpu.SemaphoreType.DMA((TILES,)),
            pltpu.SemaphoreType.DMA((7,)),
            pltpu.SemaphoreType.DMA((5,)),
        ],
        compiler_params=pltpu.CompilerParams(
            collective_id=0, has_side_effects=True, vmem_limit_bytes=48 * 2**20
        ),
        cost_estimate=pl.CostEstimate(
            flops=8 * 1024**3, bytes_accessed=4 * 2**20, transcendentals=0
        ),
    )(embeddings)
    return jnp.transpose(tiles_t)


def solution(mesh):
    return jax.shard_map(
        body,
        mesh=mesh,
        in_specs=(P(("blk", "grp"), None),),
        out_specs=P(("blk", "grp"), None),
        check_vma=False,
    )
```

```python
import jax
import jax.numpy as jnp
from jax import lax
from jax.experimental import pallas as pl
from jax.experimental.pallas import tpu as pltpu
from jax.sharding import PartitionSpec as P

MESH = pl.DeviceIdType.MESH
ROWS = 1024
TILE = 128
TILES = ROWS // TILE
UNIT = 256
UNITS = ROWS // UNIT
PIECE = 64
PIECES = ROWS // PIECE
AROUND = 5
SEAM_AROUND = 10
GRP = 2
BLOCKS = 256


def where_of(block):
    block = lax.rem(block + BLOCKS, BLOCKS)
    return (lax.div(block, GRP), lax.rem(block, GRP))


def both(*conditions):
    out = conditions[0]
    for condition in conditions[1:]:
        out = jnp.logical_and(out, condition)
    return out


def kernel(
    x_ref,
    out_ref,
    raw,
    unit,
    near,
    far,
    extra,
    pass_on,
    ring,
    back,
    load_sem,
    near_send,
    near_sem,
    ring_send,
    ring_sem,
    far_send,
    far_sem,
    extra_send,
    extra_sem,
    pass_sem,
    pass_send,
    back_send,
    back_sem,
    hello,
):
    b = lax.axis_index("blk") * GRP + lax.axis_index("grp")
    m = lax.rem(b, 4)
    z = lax.rem(lax.div(b, 4), 8)
    x = lax.rem(lax.div(b, 32), 4)
    half = lax.div(b, 128)
    y = half * 2 + lax.rem(b, 2)
    scale = 1.0 / 1024**0.5

    def at_y(offset):
        to = lax.rem(y + offset + 4, 4)
        return lax.div(to, 2) * 128 + lax.rem(b, 128) - lax.rem(b, 2) + lax.rem(to, 2)

    is_e = x >= 1
    s = jnp.where(is_e, -1, 1)
    role = jnp.where(is_e, 3 - m, m)
    even = lax.rem(role, 2) == 0
    odd = jnp.logical_not(even)
    low = m < 2
    high = jnp.logical_not(low)
    first_o = both(x == 0, z == 0)
    last_o = both(x == 0, z == 7)
    last_e = both(x == 3, z == 7)

    mate = b + 1 - 2 * lax.rem(m, 2)
    ahead = at_y(s)
    behind = at_y(-s)
    no_far = both(last_o, high)
    has_far = jnp.logical_not(no_far)
    no_send = jnp.logical_or(both(first_o, low), both(last_e, high))
    sends_far = jnp.logical_not(no_send)
    cross_e = both(last_e, m == 3)
    cross_o = both(first_o, m == 0)
    cross = jnp.logical_or(cross_e, cross_o)
    pass_e = both(last_e, m == 2)
    pass_o = both(first_o, m == 1)
    passes = jnp.logical_or(pass_e, pass_o)
    over = jnp.where(is_e, b + 1, b - 1)
    seam_e = half * 128 + 127
    seam_o = half * 128
    slow = both(last_e, low)
    around = jnp.where(last_e, jnp.where(low, SEAM_AROUND, 0), AROUND)
    direct = PIECES - around

    load = pltpu.make_async_copy(x_ref, raw, load_sem)
    load.start()

    barrier = pltpu.get_barrier_semaphore()

    def greet(condition, *blocks):
        def send():
            for block in blocks:
                pl.semaphore_signal(
                    barrier, inc=1, device_id=where_of(block), device_id_type=MESH
                )

        if condition is None:
            send()
        else:
            pl.when(condition)(send)

    greet(None, behind)
    greet(even, mate)
    greet(has_far, b + 2 * s)
    greet(cross_o, half * 128 + 126, over)
    greet(pass_o, seam_e, at_y(1))
    greet(pass_e, at_y(-1))

    def one(condition):
        return condition.astype(jnp.int32)

    pl.semaphore_wait(
        barrier,
        1
        + one(odd)
        + one(sends_far)
        + one(no_far)
        + 3 * one(cross_e)
        + one(pass_e)
        + one(cross_o),
    )

    @pl.when(cross_e)
    def _():
        for block in (over, seam_o + 1):
            pl.semaphore_signal(hello, inc=1, device_id=where_of(block), device_id_type=MESH)

    load.wait()

    def tile_rows(t, size):
        return pl.ds(pl.multiple_of(t * size, size), size)

    def around_piece(i):
        usual = jnp.where(i == 0, 7, jnp.where(i < 3, i + 9, i + 11))
        return jnp.where(slow, i, usual)

    def direct_piece(j):
        usual = jnp.where(j < 7, j, jnp.where(j < 9, j + 1, j + 3))
        return jnp.where(slow, j + SEAM_AROUND, jnp.where(last_e, j, usual))

    def remote(src, dst, send, recv, block):
        return pltpu.make_async_remote_copy(
            src_ref=src,
            dst_ref=dst,
            send_sem=send,
            recv_sem=recv,
            device_id=where_of(block),
            device_id_type=MESH,
        )

    def leg_one(i):
        p = around_piece(i)
        return remote(
            raw.at[tile_rows(p, PIECE)],
            ring.at[tile_rows(i, PIECE)],
            near_send.at[p],
            ring_sem.at[i],
            ahead,
        )

    def straight(j):
        p = direct_piece(j)
        rows = tile_rows(p, PIECE)
        return remote(raw.at[rows], near.at[rows], near_send.at[p], near_sem.at[p], mate)

    def leg_two(i):
        rows = tile_rows(i, PIECE)
        return remote(ring.at[rows], ring.at[rows], ring_send.at[i], ring_sem.at[i], ahead)

    def leg_three(i):
        p = around_piece(i)
        return remote(
            ring.at[tile_rows(i, PIECE)],
            near.at[tile_rows(p, PIECE)],
            ring_send.at[i],
            near_sem.at[p],
            ahead,
        )

    def far_copy(which, t, block):
        rows = tile_rows(t, TILE)
        return remote(raw.at[rows], far.at[rows], far_send.at[which, t], far_sem.at[t], block)

    def seam_copy(t, block):
        rows = tile_rows(t, TILE)
        return remote(raw.at[rows], pass_on.at[rows], extra_send.at[t], pass_sem.at[t], block)

    def seam_pass(t, block):
        rows = tile_rows(t, TILE)
        return remote(pass_on.at[rows], extra.at[rows], pass_send.at[t], extra_sem.at[t], block)

    def each(count, body):
        def step(t, carry):
            body(t)
            return carry

        lax.fori_loop(0, count, step, 0)

    seam_to = jnp.where(cross_e, at_y(1), at_y(-1))
    pass_to = jnp.where(pass_e, seam_o, seam_e)

    @pl.when(odd)
    def _():
        each(around, lambda i: leg_one(i).start())

        @pl.when(jnp.logical_not(slow))
        def _():
            each(direct, lambda j: straight(j).start())

    @pl.when(sends_far)
    def _():
        each(TILES, lambda t: far_copy(0, t, b - 2 * s).start())

    @pl.when(no_far)
    def _():
        each(TILES, lambda t: far_copy(1, t, b + 2 * s).start())

    @pl.when(cross)
    def _():
        each(TILES, lambda t: seam_copy(t, seam_to).start())

    def normalise(src, dst, u):
        def step(k, carry):
            rows = pl.ds(pl.multiple_of(u * UNIT + k * 32, 32), 32)
            values = src[rows, :].astype(jnp.float32)
            mean = jnp.mean(values * values, axis=-1, keepdims=True)
            dst[rows, :] = (values * lax.rsqrt(mean + 1e-06)).astype(jnp.bfloat16)
            return carry

        lax.fori_loop(0, UNIT // 32, step, 0)

    each(UNITS, lambda u: normalise(raw, unit, u))

    def scores(left, right):
        return lax.dot_general(
            left, right, (((1,), (1,)), ((), ())), preferred_element_type=jnp.float32
        )

    def own_unit(u):
        left = unit[tile_rows(u, UNIT), :]
        for n in range(UNITS):
            span = slice(n * UNIT, n * UNIT + UNIT)
            block = scores(left, unit[span, :])
            at = lax.broadcasted_iota(jnp.int32, (UNIT, UNIT), 0) + u * UNIT
            to = lax.broadcasted_iota(jnp.int32, (UNIT, UNIT), 1) + n * UNIT
            block = jnp.where(at == to, -jnp.inf, block)
            for q in range(UNIT // TILE):
                out_ref[pl.ds(16 + 2 * u + q, 1), span] = (
                    jnp.max(block[q * TILE : q * TILE + TILE, :], axis=0, keepdims=True) * scale
                )

    def pair_unit(keys_ref, rows_ref, u, by_row, row_base, by_key, key_base):
        left = keys_ref[tile_rows(u, UNIT), :]
        for n in range(UNITS):
            span = slice(n * UNIT, n * UNIT + UNIT)
            block = scores(left, rows_ref[span, :])
            for q in range(UNIT // TILE):
                part = block[q * TILE : q * TILE + TILE, :]
                by_row[pl.ds(row_base + 2 * u + q, 1), span] = (
                    jnp.max(part, axis=0, keepdims=True) * scale
                )
                columns = pl.ds(pl.multiple_of(u * UNIT + q * TILE, TILE), TILE)
                for h in range(UNIT // TILE):
                    turned = jnp.transpose(part[:, h * TILE : h * TILE + TILE])
                    by_key[pl.ds(key_base + 2 * n + h, 1), columns] = (
                        jnp.max(turned, axis=0, keepdims=True) * scale
                    )

    def slot(offset):
        return pl.multiple_of((offset + 2) * TILES, TILES)

    def take(ref, sems, u, size):
        for k in range(UNIT // size):
            t = u * (UNIT // size) + k
            rows = tile_rows(t, size)
            pltpu.make_async_copy(raw.at[rows], ref.at[rows], sems.at[t]).wait()
        normalise(ref, ref, u)

    def message(k, block, offset):
        return remote(
            back.at[pl.ds(k * TILES, TILES)],
            out_ref.at[pl.ds(slot(offset), TILES)],
            back_send.at[k],
            back_sem.at[offset + 2],
            block,
        )

    def far_unit(u):
        take(far, far_sem, u, TILE)
        pair_unit(far, unit, u, out_ref, slot(2 * s), back, 0)

    def near_unit(u):
        take(near, near_sem, u, PIECE)
        pair_unit(near, unit, u, out_ref, slot(s), back, TILES)

    def near_far_unit(u):
        pair_unit(near, far, u, back, 2 * TILES, back, 3 * TILES)

    def step(i):
        @pl.when(i < around)
        def _():
            rows = tile_rows(i, PIECE)
            pltpu.make_async_copy(raw.at[rows], ring.at[rows], ring_sem.at[i]).wait()

            @pl.when(even)
            def _():
                leg_two(i).start()

            @pl.when(odd)
            def _():
                leg_three(i).start()

        @pl.when(both(passes, i < TILES))
        def _():
            @pl.when(both(pass_o, i == 0))
            def _():
                pl.semaphore_wait(hello, 1)

            rows = tile_rows(i, TILE)
            pltpu.make_async_copy(raw.at[rows], pass_on.at[rows], pass_sem.at[i]).wait()
            seam_pass(i, pass_to).start()

        @pl.when(i < UNITS)
        def _():
            own_unit(i)

        turn = both(lax.rem(i, 2) == 1, i < 2 * UNITS)

        @pl.when(both(has_far, turn))
        def _():
            far_unit(lax.div(i, 2))

        @pl.when(both(even, jnp.logical_not(slow), jnp.logical_or(i == 4, i == 8)))
        def _():
            near_unit(lax.div(i, 4) - 1)

        @pl.when(both(cross_e, lax.rem(i, 2) == 0, i >= 2))
        def _():
            u = lax.div(i, 2) - 1
            take(extra, extra_sem, u, TILE)
            pair_unit(extra, unit, u, out_ref, slot(1), back, 4 * TILES)

    each(10, step)

    @pl.when(slow)
    def _():
        @pl.when(odd)
        def _():
            each(direct, lambda j: straight(j).start())

    @pl.when(has_far)
    def _():
        message(0, b + 2 * s, -2 * s).start()

    @pl.when(cross_e)
    def _():
        message(4, over, -1).start()
        near_unit(2)
        near_unit(3)
        each(UNITS, lambda u: pair_unit(extra, near, u, back, 5 * TILES, back, 6 * TILES))
        message(5, mate, 2).start()
        message(6, over, -2).start()
        each(UNITS, near_far_unit)

    @pl.when(both(even, jnp.logical_not(cross_e)))
    def _():
        done = jnp.where(slow, 0, 2)

        @pl.when(has_far)
        def _():
            each(done, near_far_unit)

        def rest(k):
            near_unit(done + k)

            @pl.when(has_far)
            def _():
                near_far_unit(done + k)

        each(UNITS - done, rest)

    @pl.when(even)
    def _():
        message(1, mate, -s).start()

        @pl.when(has_far)
        def _():
            message(2, b + 2 * s, -s).start()
            message(3, mate, s).start()

    @pl.when(cross_o)
    def _():
        def seam_unit(u):
            take(extra, extra_sem, u, TILE)
            pair_unit(extra, near, u, back, 5 * TILES, back, 6 * TILES)

        each(UNITS, seam_unit)
        message(5, mate, -2).start()
        pl.semaphore_wait(hello, 1)
        message(6, over, 2).start()

    def landed(offset):
        pltpu.make_async_copy(
            back.at[pl.ds(0, TILES)],
            out_ref.at[pl.ds(slot(offset), TILES)],
            back_sem.at[offset + 2],
        ).wait()

    landed(-2 * s)

    @pl.when(jnp.logical_not(cross_e))
    def _():
        landed(-s)

    @pl.when(odd)
    def _():
        landed(s)

    @pl.when(no_far)
    def _():
        landed(2 * s)

    @pl.when(odd)
    def _():
        each(around, lambda i: leg_one(i).wait_send())
        each(direct, lambda j: straight(j).wait_send())
        each(around, lambda i: leg_three(i).wait_send())

    @pl.when(even)
    def _():
        each(around, lambda i: leg_two(i).wait_send())

    @pl.when(sends_far)
    def _():
        each(TILES, lambda t: far_copy(0, t, b - 2 * s).wait_send())

    @pl.when(no_far)
    def _():
        each(TILES, lambda t: far_copy(1, t, b + 2 * s).wait_send())

    @pl.when(cross)
    def _():
        each(TILES, lambda t: seam_copy(t, seam_to).wait_send())

    @pl.when(passes)
    def _():
        each(TILES, lambda t: seam_pass(t, pass_to).wait_send())

    @pl.when(has_far)
    def _():
        message(0, b + 2 * s, -2 * s).wait_send()

    @pl.when(even)
    def _():
        message(1, mate, -s).wait_send()

        @pl.when(has_far)
        def _():
            message(2, b + 2 * s, -s).wait_send()
            message(3, mate, s).wait_send()

    @pl.when(cross_e)
    def _():
        message(4, over, -1).wait_send()

    @pl.when(cross)
    def _():
        message(5, mate, 2 * s).wait_send()
        message(6, over, 2 * s).wait_send()


def body(embeddings):
    rows, width = embeddings.shape
    block = pltpu.VMEM((rows, width), jnp.bfloat16)
    dma = pltpu.SemaphoreType.DMA
    tiles_t = pl.pallas_call(
        kernel,
        name="cycle_tile_max",
        out_shape=jax.ShapeDtypeStruct((5 * TILES, rows), jnp.float32),
        in_specs=[pl.BlockSpec(memory_space=pltpu.HBM)],
        out_specs=pl.BlockSpec(memory_space=pltpu.VMEM),
        scratch_shapes=[
            block,
            block,
            block,
            block,
            block,
            block,
            pltpu.VMEM((SEAM_AROUND * PIECE, width), jnp.bfloat16),
            pltpu.VMEM((7 * TILES, rows), jnp.float32),
            dma,
            dma((PIECES,)),
            dma((PIECES,)),
            dma((SEAM_AROUND,)),
            dma((SEAM_AROUND,)),
            dma((2, TILES)),
            dma((TILES,)),
            dma((TILES,)),
            dma((TILES,)),
            dma((TILES,)),
            dma((TILES,)),
            dma((7,)),
            dma((5,)),
            pltpu.SemaphoreType.REGULAR,
        ],
        compiler_params=pltpu.CompilerParams(
            collective_id=0, has_side_effects=True, vmem_limit_bytes=62 * 2**20 + 2**18
        ),
        cost_estimate=pl.CostEstimate(
            flops=8 * 1024**3, bytes_accessed=4 * 2**20, transcendentals=0
        ),
    )(embeddings)
    return jnp.transpose(tiles_t)


def solution(mesh):
    return jax.shard_map(
        body,
        mesh=mesh,
        in_specs=(P(("blk", "grp"), None),),
        out_specs=P(("blk", "grp"), None),
        check_vma=False,
    )
```

```python
import jax
import jax.numpy as jnp
from jax import lax
from jax.experimental import pallas as pl
from jax.experimental.pallas import tpu as pltpu
from jax.sharding import PartitionSpec as P

MESH = pl.DeviceIdType.MESH
ROWS = 1024
TILE = 128
TILES = ROWS // TILE
UNIT = 256
UNITS = ROWS // UNIT
PIECE = 64
PIECES = ROWS // PIECE
AROUND = 5
SEAM_AROUND = 10
GRP = 2
BLOCKS = 256


def where_of(block):
    block = lax.rem(block + BLOCKS, BLOCKS)
    return (lax.div(block, GRP), lax.rem(block, GRP))


def both(*conditions):
    out = conditions[0]
    for condition in conditions[1:]:
        out = jnp.logical_and(out, condition)
    return out


def kernel(
    x_ref,
    out_ref,
    raw,
    unit,
    near,
    far,
    extra,
    pass_on,
    ring,
    back,
    load_sem,
    near_send,
    near_sem,
    ring_send,
    ring_sem,
    far_send,
    far_sem,
    extra_send,
    extra_sem,
    pass_sem,
    pass_send,
    back_send,
    back_sem,
    hello,
):
    b = lax.axis_index("blk") * GRP + lax.axis_index("grp")
    m = lax.rem(b, 4)
    z = lax.rem(lax.div(b, 4), 8)
    x = lax.rem(lax.div(b, 32), 4)
    half = lax.div(b, 128)
    y = half * 2 + lax.rem(b, 2)
    scale = 1.0 / 1024**0.5

    def at_y(offset):
        to = lax.rem(y + offset + 4, 4)
        return lax.div(to, 2) * 128 + lax.rem(b, 128) - lax.rem(b, 2) + lax.rem(to, 2)

    is_e = x >= 1
    s = jnp.where(is_e, -1, 1)
    role = jnp.where(is_e, 3 - m, m)
    even = lax.rem(role, 2) == 0
    odd = jnp.logical_not(even)
    low = m < 2
    high = jnp.logical_not(low)
    first_o = both(x == 0, z == 0)
    last_o = both(x == 0, z == 7)
    last_e = both(x == 3, z == 7)

    mate = b + 1 - 2 * lax.rem(m, 2)
    ahead = at_y(s)
    behind = at_y(-s)
    no_far = both(last_o, high)
    has_far = jnp.logical_not(no_far)
    no_send = jnp.logical_or(both(first_o, low), both(last_e, high))
    sends_far = jnp.logical_not(no_send)
    cross_e = both(last_e, m == 3)
    cross_o = both(first_o, m == 0)
    cross = jnp.logical_or(cross_e, cross_o)
    pass_e = both(last_e, m == 2)
    pass_o = both(first_o, m == 1)
    passes = jnp.logical_or(pass_e, pass_o)
    over = jnp.where(is_e, b + 1, b - 1)
    seam_e = half * 128 + 127
    seam_o = half * 128
    slow = both(last_e, low)
    around = jnp.where(last_e, jnp.where(low, SEAM_AROUND, 0), AROUND)
    direct = PIECES - around

    load = pltpu.make_async_copy(x_ref, raw, load_sem)
    load.start()

    barrier = pltpu.get_barrier_semaphore()

    def greet(condition, *blocks):
        def send():
            for block in blocks:
                pl.semaphore_signal(
                    barrier, inc=1, device_id=where_of(block), device_id_type=MESH
                )

        if condition is None:
            send()
        else:
            pl.when(condition)(send)

    greet(None, behind)
    greet(even, mate)
    greet(has_far, b + 2 * s)
    greet(cross_o, half * 128 + 126, over)
    greet(pass_o, seam_e, at_y(1))
    greet(pass_e, at_y(-1))

    def one(condition):
        return condition.astype(jnp.int32)

    with jax.named_scope("bar"):
        pl.semaphore_wait(
            barrier,
            1
            + one(odd)
            + one(sends_far)
            + one(no_far)
            + 3 * one(cross_e)
            + one(pass_e)
            + one(cross_o),
        )

    @pl.when(cross_e)
    def _():
        for block in (over, seam_o + 1):
            pl.semaphore_signal(hello, inc=1, device_id=where_of(block), device_id_type=MESH)

    with jax.named_scope("load"):
        load.wait()

    def tile_rows(t, size):
        return pl.ds(pl.multiple_of(t * size, size), size)

    def around_piece(i):
        usual = jnp.where(i == 0, 7, jnp.where(i < 3, i + 9, i + 11))
        return jnp.where(slow, i, usual)

    def direct_piece(j):
        usual = jnp.where(j < 7, j, jnp.where(j < 9, j + 1, j + 3))
        return jnp.where(slow, j + SEAM_AROUND, jnp.where(last_e, j, usual))

    def remote(src, dst, send, recv, block):
        return pltpu.make_async_remote_copy(
            src_ref=src,
            dst_ref=dst,
            send_sem=send,
            recv_sem=recv,
            device_id=where_of(block),
            device_id_type=MESH,
        )

    def leg_one(i):
        p = around_piece(i)
        return remote(
            raw.at[tile_rows(p, PIECE)],
            ring.at[tile_rows(i, PIECE)],
            near_send.at[p],
            ring_sem.at[i],
            ahead,
        )

    def straight(j):
        p = direct_piece(j)
        rows = tile_rows(p, PIECE)
        return remote(raw.at[rows], near.at[rows], near_send.at[p], near_sem.at[p], mate)

    def leg_two(i):
        rows = tile_rows(i, PIECE)
        return remote(ring.at[rows], ring.at[rows], ring_send.at[i], ring_sem.at[i], ahead)

    def leg_three(i):
        p = around_piece(i)
        return remote(
            ring.at[tile_rows(i, PIECE)],
            near.at[tile_rows(p, PIECE)],
            ring_send.at[i],
            near_sem.at[p],
            ahead,
        )

    def far_copy(which, t, block):
        rows = tile_rows(t, TILE)
        return remote(raw.at[rows], far.at[rows], far_send.at[which, t], far_sem.at[t], block)

    def seam_copy(t, block):
        rows = tile_rows(t, PIECE)
        return remote(raw.at[rows], pass_on.at[rows], extra_send.at[t], pass_sem.at[t], block)

    def seam_pass(t, block):
        rows = tile_rows(t, PIECE)
        return remote(pass_on.at[rows], extra.at[rows], pass_send.at[t], extra_sem.at[t], block)

    def each(count, body):
        def step(t, carry):
            body(t)
            return carry

        lax.fori_loop(0, count, step, 0)

    seam_to = jnp.where(cross_e, at_y(1), at_y(-1))
    pass_to = jnp.where(pass_e, seam_o, seam_e)

    @pl.when(odd)
    def _():
        each(around, lambda i: leg_one(i).start())

        @pl.when(jnp.logical_not(slow))
        def _():
            each(direct, lambda j: straight(j).start())

    @pl.when(sends_far)
    def _():
        each(TILES, lambda t: far_copy(0, t, b - 2 * s).start())

    @pl.when(no_far)
    def _():
        each(TILES, lambda t: far_copy(1, t, b + 2 * s).start())

    @pl.when(cross)
    def _():
        each(PIECES, lambda t: seam_copy(t, seam_to).start())

    def normalise(src, dst, u):
        for k in range(UNIT // 64):
            rows = pl.ds(pl.multiple_of(u * UNIT + k * 64, 64), 64)
            values = src[rows, :].astype(jnp.float32)
            mean = jnp.mean(values * values, axis=-1, keepdims=True)
            dst[rows, :] = (values * lax.rsqrt(mean + 1e-06)).astype(jnp.bfloat16)

    with jax.named_scope("norm"):
        each(UNITS, lambda u: normalise(raw, unit, u))

    def scores(left, right):
        return lax.dot_general(
            left, right, (((1,), (1,)), ((), ())), preferred_element_type=jnp.float32
        )

    def own_unit(u):
        left = unit[tile_rows(u, UNIT), :]
        for n in range(UNITS):
            span = slice(n * UNIT, n * UNIT + UNIT)
            block = scores(left, unit[span, :])
            at = lax.broadcasted_iota(jnp.int32, (UNIT, UNIT), 0) + u * UNIT
            to = lax.broadcasted_iota(jnp.int32, (UNIT, UNIT), 1) + n * UNIT
            block = jnp.where(at == to, -jnp.inf, block)
            for q in range(UNIT // TILE):
                out_ref[pl.ds(16 + 2 * u + q, 1), span] = (
                    jnp.max(block[q * TILE : q * TILE + TILE, :], axis=0, keepdims=True) * scale
                )

    def pair_unit(keys_ref, rows_ref, u, by_row, row_base, by_key, key_base):
        left = keys_ref[tile_rows(u, UNIT), :]
        for n in range(UNITS):
            span = slice(n * UNIT, n * UNIT + UNIT)
            block = scores(left, rows_ref[span, :])
            for q in range(UNIT // TILE):
                part = block[q * TILE : q * TILE + TILE, :]
                by_row[pl.ds(row_base + 2 * u + q, 1), span] = (
                    jnp.max(part, axis=0, keepdims=True) * scale
                )
                columns = pl.ds(pl.multiple_of(u * UNIT + q * TILE, TILE), TILE)
                for h in range(UNIT // TILE):
                    turned = jnp.transpose(part[:, h * TILE : h * TILE + TILE])
                    by_key[pl.ds(key_base + 2 * n + h, 1), columns] = (
                        jnp.max(turned, axis=0, keepdims=True) * scale
                    )

    def slot(offset):
        return pl.multiple_of((offset + 2) * TILES, TILES)

    def take(ref, sems, u, size):
        for k in range(UNIT // size):
            t = u * (UNIT // size) + k
            rows = tile_rows(t, size)
            pltpu.make_async_copy(raw.at[rows], ref.at[rows], sems.at[t]).wait()
        normalise(ref, ref, u)

    def message(k, block, offset):
        return remote(
            back.at[pl.ds(k * TILES, TILES)],
            out_ref.at[pl.ds(slot(offset), TILES)],
            back_send.at[k],
            back_sem.at[offset + 2],
            block,
        )

    def far_unit(u):
        with jax.named_scope("farw"):
            take(far, far_sem, u, TILE)
        with jax.named_scope("farc"):
            pair_unit(far, unit, u, out_ref, slot(2 * s), back, 0)

    def near_unit(u):
        with jax.named_scope("nearw"):
            take(near, near_sem, u, PIECE)
        with jax.named_scope("nearc"):
            pair_unit(near, unit, u, out_ref, slot(s), back, TILES)

    def near_far_unit(u):
        with jax.named_scope("nfc"):
            pair_unit(near, far, u, back, 2 * TILES, back, 3 * TILES)

    def extra_unit(u):
        with jax.named_scope("xw"):
            take(extra, extra_sem, u, PIECE)
        with jax.named_scope("xuc"):
            pair_unit(extra, unit, u, out_ref, slot(1), back, 4 * TILES)

    def extra_near_unit(u):
        with jax.named_scope("xnc"):
            pair_unit(extra, near, u, back, 5 * TILES, back, 6 * TILES)

    def forward(i):
        @pl.when(both(passes, i < TILES))
        def _():
            @pl.when(both(pass_o, i == 0))
            def _():
                with jax.named_scope("hello"):
                    pl.semaphore_wait(hello, 1)

            for k in range(TILE // PIECE):
                t = i * (TILE // PIECE) + k
                rows = tile_rows(t, PIECE)
                with jax.named_scope("passw"):
                    pltpu.make_async_copy(raw.at[rows], pass_on.at[rows], pass_sem.at[t]).wait()
                seam_pass(t, pass_to).start()

        @pl.when(i < around)
        def _():
            rows = tile_rows(i, PIECE)
            with jax.named_scope("ringw"):
                pltpu.make_async_copy(raw.at[rows], ring.at[rows], ring_sem.at[i]).wait()

            @pl.when(even)
            def _():
                leg_two(i).start()

            @pl.when(odd)
            def _():
                leg_three(i).start()

        @pl.when(i < UNITS)
        def _():
            with jax.named_scope("own"):
                own_unit(i)

    each(jnp.where(passes, TILES, jnp.where(slow, SEAM_AROUND, AROUND)), forward)

    @pl.when(both(slow, odd))
    def _():
        each(direct, lambda j: straight(j).start())

    def arrive(k):
        @pl.when(has_far)
        def _():
            far_unit(k)

        @pl.when(both(even, jnp.logical_not(cross_e), jnp.logical_or(k == 1, k == 2)))
        def _():
            near_unit(k - 1)

    each(UNITS, arrive)

    @pl.when(has_far)
    def _():
        message(0, b + 2 * s, -2 * s).start()

    @pl.when(both(even, jnp.logical_not(cross_e)))
    def _():
        @pl.when(has_far)
        def _():
            each(2, near_far_unit)

        def rest(k):
            near_unit(2 + k)

            @pl.when(has_far)
            def _():
                near_far_unit(2 + k)

        each(2, rest)

    @pl.when(cross_e)
    def _():
        def all_four(u):
            near_unit(u)
            near_far_unit(u)

            @pl.when(u < UNITS - 1)
            def _():
                extra_unit(u)

        each(UNITS, all_four)

    @pl.when(even)
    def _():
        message(1, mate, -s).start()

        @pl.when(has_far)
        def _():
            message(2, b + 2 * s, -s).start()
            message(3, mate, s).start()

    @pl.when(cross_e)
    def _():
        each(UNITS - 1, extra_near_unit)
        extra_unit(UNITS - 1)
        message(4, over, -1).start()
        extra_near_unit(UNITS - 1)
        message(5, mate, 2).start()
        message(6, over, -2).start()

    @pl.when(cross_o)
    def _():
        def seam_unit(u):
            with jax.named_scope("xw"):
                take(extra, extra_sem, u, PIECE)
            extra_near_unit(u)

        each(UNITS, seam_unit)
        message(5, mate, -2).start()
        pl.semaphore_wait(hello, 1)
        message(6, over, 2).start()

    def landed(offset):
        pltpu.make_async_copy(
            back.at[pl.ds(0, TILES)],
            out_ref.at[pl.ds(slot(offset), TILES)],
            back_sem.at[offset + 2],
        ).wait()

    with jax.named_scope("landed"):
        landed(-2 * s)

        @pl.when(jnp.logical_not(cross_e))
        def _():
            landed(-s)

        @pl.when(odd)
        def _():
            landed(s)

        @pl.when(no_far)
        def _():
            landed(2 * s)

    with jax.named_scope("settle"):
        @pl.when(odd)
        def _():
            each(around, lambda i: leg_one(i).wait_send())
            each(direct, lambda j: straight(j).wait_send())
            each(around, lambda i: leg_three(i).wait_send())

        @pl.when(even)
        def _():
            each(around, lambda i: leg_two(i).wait_send())

        @pl.when(sends_far)
        def _():
            each(TILES, lambda t: far_copy(0, t, b - 2 * s).wait_send())

        @pl.when(no_far)
        def _():
            each(TILES, lambda t: far_copy(1, t, b + 2 * s).wait_send())

        @pl.when(cross)
        def _():
            each(PIECES, lambda t: seam_copy(t, seam_to).wait_send())

        @pl.when(passes)
        def _():
            each(PIECES, lambda t: seam_pass(t, pass_to).wait_send())

        @pl.when(has_far)
        def _():
            message(0, b + 2 * s, -2 * s).wait_send()

        @pl.when(even)
        def _():
            message(1, mate, -s).wait_send()

            @pl.when(has_far)
            def _():
                message(2, b + 2 * s, -s).wait_send()
                message(3, mate, s).wait_send()

        @pl.when(cross_e)
        def _():
            message(4, over, -1).wait_send()

        @pl.when(cross)
        def _():
            message(5, mate, 2 * s).wait_send()
            message(6, over, 2 * s).wait_send()


def body(embeddings):
    rows, width = embeddings.shape
    block = pltpu.VMEM((rows, width), jnp.bfloat16)
    dma = pltpu.SemaphoreType.DMA
    tiles_t = pl.pallas_call(
        kernel,
        name="cycle_tile_max",
        out_shape=jax.ShapeDtypeStruct((5 * TILES, rows), jnp.float32),
        in_specs=[pl.BlockSpec(memory_space=pltpu.HBM)],
        out_specs=pl.BlockSpec(memory_space=pltpu.VMEM),
        scratch_shapes=[
            block,
            block,
            block,
            block,
            block,
            block,
            pltpu.VMEM((SEAM_AROUND * PIECE, width), jnp.bfloat16),
            pltpu.VMEM((7 * TILES, rows), jnp.float32),
            dma,
            dma((PIECES,)),
            dma((PIECES,)),
            dma((SEAM_AROUND,)),
            dma((SEAM_AROUND,)),
            dma((2, TILES)),
            dma((TILES,)),
            dma((PIECES,)),
            dma((PIECES,)),
            dma((PIECES,)),
            dma((PIECES,)),
            dma((7,)),
            dma((5,)),
            pltpu.SemaphoreType.REGULAR,
        ],
        compiler_params=pltpu.CompilerParams(
            collective_id=0, has_side_effects=True, vmem_limit_bytes=52 * 2**20
        ),
        cost_estimate=pl.CostEstimate(
            flops=8 * 1024**3, bytes_accessed=4 * 2**20, transcendentals=0
        ),
    )(embeddings)
    return jnp.transpose(tiles_t)


def solution(mesh):
    return jax.shard_map(
        body,
        mesh=mesh,
        in_specs=(P(("blk", "grp"), None),),
        out_specs=P(("blk", "grp"), None),
        check_vma=False,
    )
```

```python
import jax
import jax.numpy as jnp
from jax import lax
from jax.experimental import pallas as pl
from jax.experimental.pallas import tpu as pltpu
from jax.sharding import PartitionSpec as P

MESH = pl.DeviceIdType.MESH
ROWS = 1024
TILE = 128
TILES = ROWS // TILE
UNIT = 256
UNITS = ROWS // UNIT
PIECE = 64
PIECES = ROWS // PIECE
AROUND = 5
SEAM_AROUND = 10
LEAD = 4
GRP = 2
BLOCKS = 256


def where_of(block):
    block = lax.rem(block + BLOCKS, BLOCKS)
    return (lax.div(block, GRP), lax.rem(block, GRP))


def both(*conditions):
    out = conditions[0]
    for condition in conditions[1:]:
        out = jnp.logical_and(out, condition)
    return out


def kernel(
    x_ref,
    out_ref,
    raw,
    unit,
    near,
    far,
    extra,
    near_in,
    far_in,
    extra_in,
    pass_on,
    ring,
    back,
    load_sem,
    near_send,
    near_sem,
    ring_send,
    ring_sem,
    far_send,
    far_sem,
    extra_send,
    extra_sem,
    pass_sem,
    pass_send,
    back_send,
    back_sem,
    hello,
    far_hello,
):
    b = lax.axis_index("blk") * GRP + lax.axis_index("grp")
    m = lax.rem(b, 4)
    z = lax.rem(lax.div(b, 4), 8)
    x = lax.rem(lax.div(b, 32), 4)
    half = lax.div(b, 128)
    y = half * 2 + lax.rem(b, 2)
    scale = 1.0 / 1024**0.5

    def at_y(offset):
        to = lax.rem(y + offset + 4, 4)
        return lax.div(to, 2) * 128 + lax.rem(b, 128) - lax.rem(b, 2) + lax.rem(to, 2)

    is_e = x >= 1
    s = jnp.where(is_e, -1, 1)
    role = jnp.where(is_e, 3 - m, m)
    even = lax.rem(role, 2) == 0
    odd = jnp.logical_not(even)
    low = m < 2
    high = jnp.logical_not(low)
    first_o = both(x == 0, z == 0)
    last_o = both(x == 0, z == 7)
    last_e = both(x == 3, z == 7)

    mate = b + 1 - 2 * lax.rem(m, 2)
    ahead = at_y(s)
    behind = at_y(-s)
    no_far = both(last_o, high)
    has_far = jnp.logical_not(no_far)
    no_send = jnp.logical_or(both(first_o, low), both(last_e, high))
    sends_far = jnp.logical_not(no_send)
    cross_e = both(last_e, m == 3)
    cross_o = both(first_o, m == 0)
    cross = jnp.logical_or(cross_e, cross_o)
    pass_e = both(last_e, m == 2)
    pass_o = both(first_o, m == 1)
    passes = jnp.logical_or(pass_e, pass_o)
    over = jnp.where(is_e, b + 1, b - 1)
    seam_e = half * 128 + 127
    seam_o = half * 128
    slow = both(last_e, low)
    step_in = both(is_e, z == 0, low)
    step_out = both(is_e, z == 7, high)
    answers = both(is_e, jnp.logical_not(step_in))
    asks = both(is_e, sends_far, jnp.logical_not(step_out))
    around = jnp.where(last_e, jnp.where(low, SEAM_AROUND, 0), AROUND)
    direct = PIECES - around

    load = pltpu.make_async_copy(x_ref, raw, load_sem)
    load.start()

    barrier = pltpu.get_barrier_semaphore()

    def greet(condition, *blocks):
        def send():
            for block in blocks:
                pl.semaphore_signal(
                    barrier, inc=1, device_id=where_of(block), device_id_type=MESH
                )

        if condition is None:
            send()
        else:
            pl.when(condition)(send)

    greet(None, behind)
    greet(even, mate)
    greet(both(has_far, jnp.logical_not(answers)), b + 2 * s)
    greet(asks, b - 2 * s)
    greet(cross_o, half * 128 + 126, over)
    greet(pass_o, seam_e, at_y(1))
    greet(pass_e, at_y(-1))

    def one(condition):
        return condition.astype(jnp.int32)

    with jax.named_scope("bar"):
        pl.semaphore_wait(
            barrier,
            1
            + one(odd)
            + one(both(sends_far, jnp.logical_not(asks)))
        + one(answers)
            + one(no_far)
            + 3 * one(cross_e)
            + one(pass_e)
            + one(cross_o),
        )

    @pl.when(cross_e)
    def _():
        for block in (over, seam_o + 1):
            pl.semaphore_signal(hello, inc=1, device_id=where_of(block), device_id_type=MESH)

    @pl.when(answers)
    def _():
        pl.semaphore_signal(
            far_hello, inc=1, device_id=where_of(b + 2 * s), device_id_type=MESH
        )

    with jax.named_scope("load"):
        load.wait()

    def tile_rows(t, size):
        return pl.ds(pl.multiple_of(t * size, size), size)

    def around_piece(i):
        usual = jnp.where(i == 0, 7, jnp.where(i < 3, i + 9, i + 11))
        return jnp.where(slow, i, usual)

    def direct_piece(j):
        usual = jnp.where(j < 7, j, jnp.where(j < 9, j + 1, j + 3))
        return jnp.where(slow, j + SEAM_AROUND, jnp.where(last_e, j, usual))

    def remote(src, dst, send, recv, block):
        return pltpu.make_async_remote_copy(
            src_ref=src,
            dst_ref=dst,
            send_sem=send,
            recv_sem=recv,
            device_id=where_of(block),
            device_id_type=MESH,
        )

    def leg_one(i):
        p = around_piece(i)
        return remote(
            raw.at[tile_rows(p, PIECE)],
            ring.at[tile_rows(i, PIECE)],
            near_send.at[p],
            ring_sem.at[i],
            ahead,
        )

    def straight(j):
        p = direct_piece(j)
        rows = tile_rows(p, PIECE)
        return remote(raw.at[rows], near_in.at[rows], near_send.at[p], near_sem.at[p], mate)

    def leg_two(i):
        rows = tile_rows(i, PIECE)
        return remote(ring.at[rows], ring.at[rows], ring_send.at[i], ring_sem.at[i], ahead)

    def leg_three(i):
        p = around_piece(i)
        return remote(
            ring.at[tile_rows(i, PIECE)],
            near_in.at[tile_rows(p, PIECE)],
            ring_send.at[i],
            near_sem.at[p],
            ahead,
        )

    def far_copy(which, t, block):
        rows = tile_rows(t, TILE)
        return remote(raw.at[rows], far_in.at[rows], far_send.at[which, t], far_sem.at[t], block)

    def seam_copy(t, block):
        rows = tile_rows(t, PIECE)
        return remote(raw.at[rows], pass_on.at[rows], extra_send.at[t], pass_sem.at[t], block)

    def seam_pass(t, block):
        rows = tile_rows(t, PIECE)
        return remote(pass_on.at[rows], extra_in.at[rows], pass_send.at[t], extra_sem.at[t], block)

    def each(count, body):
        def step(t, carry):
            body(t)
            return carry

        lax.fori_loop(0, count, step, 0)

    seam_to = jnp.where(cross_e, at_y(1), at_y(-1))
    pass_to = jnp.where(pass_e, seam_o, seam_e)

    @pl.when(odd)
    def _():
        each(around, lambda i: leg_one(i).start())

        @pl.when(jnp.logical_not(slow))
        def _():
            each(direct, lambda j: straight(j).start())

    @pl.when(cross)
    def _():
        each(PIECES, lambda t: seam_copy(t, seam_to).start())

    def normalise(src, dst, u):
        for k in range(UNIT // 64):
            rows = pl.ds(pl.multiple_of(u * UNIT + k * 64, 64), 64)
            values = src[rows, :].astype(jnp.float32)
            mean = jnp.mean(values * values, axis=-1, keepdims=True)
            dst[rows, :] = (values * lax.rsqrt(mean + 1e-06)).astype(jnp.bfloat16)

    with jax.named_scope("norm"):
        each(UNITS, lambda u: normalise(raw, unit, u))

    @pl.when(asks)
    def _():
        with jax.named_scope("fhello"):
            pl.semaphore_wait(far_hello, 1)

    @pl.when(sends_far)
    def _():
        each(TILES, lambda t: far_copy(0, t, b - 2 * s).start())

    @pl.when(no_far)
    def _():
        each(TILES, lambda t: far_copy(1, t, b + 2 * s).start())

    def scores(left, right):
        return lax.dot_general(
            left, right, (((1,), (1,)), ((), ())), preferred_element_type=jnp.float32
        )

    def own_unit(u):
        left = unit[tile_rows(u, UNIT), :]
        for n in range(UNITS):
            span = slice(n * UNIT, n * UNIT + UNIT)
            block = scores(left, unit[span, :])
            at = lax.broadcasted_iota(jnp.int32, (UNIT, UNIT), 0) + u * UNIT
            to = lax.broadcasted_iota(jnp.int32, (UNIT, UNIT), 1) + n * UNIT
            block = jnp.where(at == to, -jnp.inf, block)
            for q in range(UNIT // TILE):
                out_ref[pl.ds(16 + 2 * u + q, 1), span] = (
                    jnp.max(block[q * TILE : q * TILE + TILE, :], axis=0, keepdims=True) * scale
                )

    def pair_unit(keys_ref, rows_ref, u, by_row, row_base, by_key, key_base):
        left = keys_ref[tile_rows(u, UNIT), :]
        for n in range(UNITS):
            span = slice(n * UNIT, n * UNIT + UNIT)
            block = scores(left, rows_ref[span, :])
            for q in range(UNIT // TILE):
                part = block[q * TILE : q * TILE + TILE, :]
                by_row[pl.ds(row_base + 2 * u + q, 1), span] = (
                    jnp.max(part, axis=0, keepdims=True) * scale
                )
                columns = pl.ds(pl.multiple_of(u * UNIT + q * TILE, TILE), TILE)
                for h in range(UNIT // TILE):
                    turned = jnp.transpose(part[:, h * TILE : h * TILE + TILE])
                    by_key[pl.ds(key_base + 2 * n + h, 1), columns] = (
                        jnp.max(turned, axis=0, keepdims=True) * scale
                    )

    def slot(offset):
        return pl.multiple_of((offset + 2) * TILES, TILES)

    def take(landing, ref, sems, u, size):
        for k in range(UNIT // size):
            t = u * (UNIT // size) + k
            rows = tile_rows(t, size)
            pltpu.make_async_copy(raw.at[rows], landing.at[rows], sems.at[t]).wait()
        normalise(landing, ref, u)

    def message(k, block, offset):
        return remote(
            back.at[pl.ds(k * TILES, TILES)],
            out_ref.at[pl.ds(slot(offset), TILES)],
            back_send.at[k],
            back_sem.at[offset + 2],
            block,
        )

    def far_unit(u):
        with jax.named_scope("farw"):
            take(far_in, far, far_sem, u, TILE)
        with jax.named_scope("farc"):
            pair_unit(far, unit, u, out_ref, slot(2 * s), back, 0)

    def near_take(u):
        with jax.named_scope("nearw"):
            take(near_in, near, near_sem, u, PIECE)

    def near_score(u):
        with jax.named_scope("nearc"):
            pair_unit(near, unit, u, out_ref, slot(s), back, TILES)

    def near_unit(u):
        near_take(u)
        near_score(u)

    def near_far_unit(u):
        with jax.named_scope("nfc"):
            pair_unit(near, far, u, back, 2 * TILES, back, 3 * TILES)

    def extra_take(u):
        with jax.named_scope("xw"):
            take(extra_in, extra, extra_sem, u, PIECE)

    def extra_unit(u):
        extra_take(u)
        with jax.named_scope("xuc"):
            pair_unit(extra, unit, u, out_ref, slot(1), back, 4 * TILES)

    def extra_near_unit(u):
        with jax.named_scope("xnc"):
            pair_unit(extra, near, u, back, 5 * TILES, back, 6 * TILES)

    def seam_forward(t):
        rows = tile_rows(t, PIECE)
        with jax.named_scope("passw"):
            pltpu.make_async_copy(raw.at[rows], pass_on.at[rows], pass_sem.at[t]).wait()
        seam_pass(t, pass_to).start()

    @pl.when(passes)
    def _():
        @pl.when(pass_o)
        def _():
            with jax.named_scope("hello"):
                pl.semaphore_wait(hello, 1)

        each(LEAD, seam_forward)

    def forward(i):
        @pl.when(both(passes, i < (PIECES - LEAD) // 2))
        def _():
            seam_forward(LEAD + 2 * i)
            seam_forward(LEAD + 2 * i + 1)

        @pl.when(i < around)
        def _():
            rows = tile_rows(i, PIECE)
            with jax.named_scope("ringw"):
                pltpu.make_async_copy(raw.at[rows], ring.at[rows], ring_sem.at[i]).wait()

            @pl.when(even)
            def _():
                leg_two(i).start()

            @pl.when(odd)
            def _():
                leg_three(i).start()

        @pl.when(both(slow, odd, i == 8))
        def _():
            each(direct, lambda j: straight(j).start())

        @pl.when(i < UNITS)
        def _():
            with jax.named_scope("own"):
                own_unit(i)

    each(jnp.where(passes, (PIECES - LEAD) // 2, jnp.where(slow, SEAM_AROUND, AROUND)), forward)

    plain = both(even, jnp.logical_not(cross_e))

    def arrive(k):
        @pl.when(both(even, step_in, k == 3))
        def _():
            near_unit(2)

        @pl.when(has_far)
        def _():
            far_unit(k)

        @pl.when(both(plain, jnp.logical_or(k == 1, k == 2)))
        def _():
            near_unit(k - 1)

    each(UNITS, arrive)

    @pl.when(has_far)
    def _():
        message(0, b + 2 * s, -2 * s).start()

    @pl.when(plain)
    def _():
        def rest(k):
            @pl.when(both(k == 2, jnp.logical_not(step_in)))
            def _():
                near_unit(2)

            @pl.when(both(cross_o, k == 2))
            def _():
                extra_take(0)
                extra_take(1)

            @pl.when(k == 3)
            def _():
                near_take(3)

            @pl.when(has_far)
            def _():
                near_far_unit(k)

        each(UNITS, rest)

        @pl.when(has_far)
        def _():
            message(2, b + 2 * s, -s).start()
            message(3, mate, s).start()

        near_score(3)
        message(1, mate, -s).start()

    @pl.when(cross_e)
    def _():
        def all_four(u):
            near_unit(u)
            near_far_unit(u)

            @pl.when(u < UNITS - 1)
            def _():
                extra_unit(u)

        each(UNITS, all_four)
        message(2, b + 2 * s, -s).start()
        message(3, mate, s).start()
        message(1, mate, -s).start()

    @pl.when(cross_e)
    def _():
        each(UNITS - 1, extra_near_unit)
        extra_unit(UNITS - 1)
        message(4, over, -1).start()
        extra_near_unit(UNITS - 1)
        message(5, mate, 2).start()
        message(6, over, -2).start()

    @pl.when(cross_o)
    def _():
        def seam_unit(u):
            @pl.when(u >= 2)
            def _():
                extra_take(u)

            extra_near_unit(u)

        each(UNITS, seam_unit)
        message(5, mate, -2).start()
        pl.semaphore_wait(hello, 1)
        message(6, over, 2).start()

    def landed(offset):
        pltpu.make_async_copy(
            back.at[pl.ds(0, TILES)],
            out_ref.at[pl.ds(slot(offset), TILES)],
            back_sem.at[offset + 2],
        ).wait()

    with jax.named_scope("landed"):
        landed(-2 * s)

        @pl.when(jnp.logical_not(cross_e))
        def _():
            landed(-s)

        @pl.when(odd)
        def _():
            landed(s)

        @pl.when(no_far)
        def _():
            landed(2 * s)

    with jax.named_scope("settle"):
        @pl.when(odd)
        def _():
            each(around, lambda i: leg_one(i).wait_send())
            each(direct, lambda j: straight(j).wait_send())
            each(around, lambda i: leg_three(i).wait_send())

        @pl.when(even)
        def _():
            each(around, lambda i: leg_two(i).wait_send())

        @pl.when(sends_far)
        def _():
            each(TILES, lambda t: far_copy(0, t, b - 2 * s).wait_send())

        @pl.when(no_far)
        def _():
            each(TILES, lambda t: far_copy(1, t, b + 2 * s).wait_send())

        @pl.when(cross)
        def _():
            each(PIECES, lambda t: seam_copy(t, seam_to).wait_send())

        @pl.when(passes)
        def _():
            each(PIECES, lambda t: seam_pass(t, pass_to).wait_send())

        @pl.when(has_far)
        def _():
            message(0, b + 2 * s, -2 * s).wait_send()

        @pl.when(even)
        def _():
            message(1, mate, -s).wait_send()

            @pl.when(has_far)
            def _():
                message(2, b + 2 * s, -s).wait_send()
                message(3, mate, s).wait_send()

        @pl.when(cross_e)
        def _():
            message(4, over, -1).wait_send()

        @pl.when(cross)
        def _():
            message(5, mate, 2 * s).wait_send()
            message(6, over, 2 * s).wait_send()


def body(embeddings):
    rows, width = embeddings.shape
    block = pltpu.VMEM((rows, width), jnp.bfloat16)
    dma = pltpu.SemaphoreType.DMA
    tiles_t = pl.pallas_call(
        kernel,
        name="cycle_tile_max",
        out_shape=jax.ShapeDtypeStruct((5 * TILES, rows), jnp.float32),
        in_specs=[pl.BlockSpec(memory_space=pltpu.HBM)],
        out_specs=pl.BlockSpec(memory_space=pltpu.VMEM),
        scratch_shapes=[
            block,
            block,
            block,
            block,
            block,
            block,
            block,
            block,
            block,
            pltpu.VMEM((SEAM_AROUND * PIECE, width), jnp.bfloat16),
            pltpu.VMEM((7 * TILES, rows), jnp.float32),
            dma,
            dma((PIECES,)),
            dma((PIECES,)),
            dma((SEAM_AROUND,)),
            dma((SEAM_AROUND,)),
            dma((2, TILES)),
            dma((TILES,)),
            dma((PIECES,)),
            dma((PIECES,)),
            dma((PIECES,)),
            dma((PIECES,)),
            dma((7,)),
            dma((5,)),
            pltpu.SemaphoreType.REGULAR,
            pltpu.SemaphoreType.REGULAR,
        ],
        compiler_params=pltpu.CompilerParams(
            collective_id=0, has_side_effects=True, vmem_limit_bytes=52 * 2**20
        ),
        cost_estimate=pl.CostEstimate(
            flops=8 * 1024**3, bytes_accessed=4 * 2**20, transcendentals=0
        ),
    )(embeddings)
    return jnp.transpose(tiles_t)


def solution(mesh):
    return jax.shard_map(
        body,
        mesh=mesh,
        in_specs=(P(("blk", "grp"), None),),
        out_specs=P(("blk", "grp"), None),
        check_vma=False,
    )
```

```python
import jax
import jax.numpy as jnp
from jax import lax
from jax.experimental import pallas as pl
from jax.experimental.pallas import tpu as pltpu
from jax.sharding import PartitionSpec as P

MESH = pl.DeviceIdType.MESH
ROWS = 1024
TILE = 128
TILES = ROWS // TILE
UNIT = 256
UNITS = ROWS // UNIT
PIECE = 64
PIECES = ROWS // PIECE
AROUND = 5
SEAM_AROUND = 10
LEAD = 4
GRP = 2
BLOCKS = 256


def where_of(block):
    block = lax.rem(block + BLOCKS, BLOCKS)
    return (lax.div(block, GRP), lax.rem(block, GRP))


def both(*conditions):
    out = conditions[0]
    for condition in conditions[1:]:
        out = jnp.logical_and(out, condition)
    return out


def kernel(
    x_ref,
    out_ref,
    raw,
    unit,
    near,
    far,
    extra,
    near_in,
    far_in,
    extra_in,
    pass_on,
    ring,
    back,
    load_sem,
    near_send,
    near_sem,
    ring_send,
    ring_sem,
    far_send,
    far_sem,
    extra_send,
    extra_sem,
    pass_sem,
    pass_send,
    back_send,
    back_sem,
    hello,
    far_hello,
):
    b = lax.axis_index("blk") * GRP + lax.axis_index("grp")
    m = lax.rem(b, 4)
    z = lax.rem(lax.div(b, 4), 8)
    x = lax.rem(lax.div(b, 32), 4)
    half = lax.div(b, 128)
    y = half * 2 + lax.rem(b, 2)
    scale = 1.0 / 1024**0.5

    def at_y(offset):
        to = lax.rem(y + offset + 4, 4)
        return lax.div(to, 2) * 128 + lax.rem(b, 128) - lax.rem(b, 2) + lax.rem(to, 2)

    is_e = x >= 1
    s = jnp.where(is_e, -1, 1)
    role = jnp.where(is_e, 3 - m, m)
    even = lax.rem(role, 2) == 0
    odd = jnp.logical_not(even)
    low = m < 2
    high = jnp.logical_not(low)
    first_o = both(x == 0, z == 0)
    last_o = both(x == 0, z == 7)
    last_e = both(x == 3, z == 7)

    mate = b + 1 - 2 * lax.rem(m, 2)
    ahead = at_y(s)
    behind = at_y(-s)
    no_far = both(last_o, high)
    has_far = jnp.logical_not(no_far)
    no_send = jnp.logical_or(both(first_o, low), both(last_e, high))
    sends_far = jnp.logical_not(no_send)
    cross_e = both(last_e, m == 3)
    cross_o = both(first_o, m == 0)
    cross = jnp.logical_or(cross_e, cross_o)
    pass_e = both(last_e, m == 2)
    pass_o = both(first_o, m == 1)
    passes = jnp.logical_or(pass_e, pass_o)
    over = jnp.where(is_e, b + 1, b - 1)
    seam_e = half * 128 + 127
    seam_o = half * 128
    slow = both(last_e, low)
    step_in = both(is_e, z == 0, low)
    step_out = both(is_e, z == 7, high)
    answers = both(is_e, jnp.logical_not(step_in))
    asks = both(is_e, sends_far, jnp.logical_not(step_out))
    around = jnp.where(last_e, jnp.where(low, SEAM_AROUND, 0), jnp.where(low, AROUND, AROUND + 1))
    direct = PIECES - around

    load = pltpu.make_async_copy(x_ref, raw, load_sem)
    load.start()

    barrier = pltpu.get_barrier_semaphore()

    def greet(condition, *blocks):
        def send():
            for block in blocks:
                pl.semaphore_signal(
                    barrier, inc=1, device_id=where_of(block), device_id_type=MESH
                )

        if condition is None:
            send()
        else:
            pl.when(condition)(send)

    greet(None, behind)
    greet(even, mate)
    greet(both(has_far, jnp.logical_not(answers)), b + 2 * s)
    greet(asks, b - 2 * s)
    greet(cross_o, half * 128 + 126, over)
    greet(pass_o, seam_e, at_y(1))
    greet(pass_e, at_y(-1))

    def one(condition):
        return condition.astype(jnp.int32)

    with jax.named_scope("bar"):
        pl.semaphore_wait(
            barrier,
            1
            + one(odd)
            + one(both(sends_far, jnp.logical_not(asks)))
        + one(answers)
            + one(no_far)
            + 3 * one(cross_e)
            + one(pass_e)
            + one(cross_o),
        )

    @pl.when(cross_e)
    def _():
        for block in (over, seam_o + 1):
            pl.semaphore_signal(hello, inc=1, device_id=where_of(block), device_id_type=MESH)

    @pl.when(answers)
    def _():
        pl.semaphore_signal(
            far_hello, inc=1, device_id=where_of(b + 2 * s), device_id_type=MESH
        )

    with jax.named_scope("load"):
        load.wait()

    def tile_rows(t, size):
        return pl.ds(pl.multiple_of(t * size, size), size)

    def around_piece(i):
        five = jnp.where(i < 3, i + 9, i + 11)
        six = jnp.where(i < 4, i + 8, i + 10)
        usual = jnp.where(i == 0, 7, jnp.where(low, five, six))
        return jnp.where(slow, i, usual)

    def direct_piece(j):
        five = jnp.where(j < 9, j + 1, j + 3)
        six = jnp.where(j < 8, j + 1, j + 4)
        usual = jnp.where(j < 7, j, jnp.where(low, five, six))
        return jnp.where(slow, j + SEAM_AROUND, jnp.where(last_e, j, usual))

    def remote(src, dst, send, recv, block):
        return pltpu.make_async_remote_copy(
            src_ref=src,
            dst_ref=dst,
            send_sem=send,
            recv_sem=recv,
            device_id=where_of(block),
            device_id_type=MESH,
        )

    def leg_one(i):
        p = around_piece(i)
        return remote(
            raw.at[tile_rows(p, PIECE)],
            ring.at[tile_rows(i, PIECE)],
            near_send,
            ring_sem.at[i],
            ahead,
        )

    def straight(j):
        p = direct_piece(j)
        rows = tile_rows(p, PIECE)
        return remote(raw.at[rows], near_in.at[rows], near_send, near_sem.at[lax.div(p, UNIT // PIECE)], mate)

    def leg_two(i):
        rows = tile_rows(i, PIECE)
        return remote(ring.at[rows], ring.at[rows], ring_send, ring_sem.at[i], ahead)

    def leg_three(i):
        p = around_piece(i)
        return remote(
            ring.at[tile_rows(i, PIECE)],
            near_in.at[tile_rows(p, PIECE)],
            ring_send,
            near_sem.at[lax.div(p, UNIT // PIECE)],
            ahead,
        )

    def far_copy(which, t, block):
        rows = tile_rows(t, TILE)
        return remote(raw.at[rows], far_in.at[rows], far_send.at[which], far_sem.at[lax.div(t, UNIT // TILE)], block)

    def seam_copy(t, block):
        rows = tile_rows(t, PIECE)
        return remote(raw.at[rows], pass_on.at[rows], extra_send, pass_sem.at[t], block)

    def seam_pass(t, block):
        rows = tile_rows(t, PIECE)
        return remote(pass_on.at[rows], extra_in.at[rows], pass_send, extra_sem.at[lax.div(t, UNIT // PIECE)], block)

    def each(count, body):
        def step(t, carry):
            body(t)
            return carry

        lax.fori_loop(0, count, step, 0)

    seam_to = jnp.where(cross_e, at_y(1), at_y(-1))
    pass_to = jnp.where(pass_e, seam_o, seam_e)

    @pl.when(odd)
    def _():
        each(around, lambda i: leg_one(i).start())

        @pl.when(jnp.logical_not(slow))
        def _():
            each(direct, lambda j: straight(j).start())

    @pl.when(cross)
    def _():
        each(PIECES, lambda t: seam_copy(t, seam_to).start())

    def normalise(src, dst, u):
        for k in range(UNIT // 64):
            rows = pl.ds(pl.multiple_of(u * UNIT + k * 64, 64), 64)
            values = src[rows, :].astype(jnp.float32)
            mean = jnp.mean(values * values, axis=-1, keepdims=True)
            dst[rows, :] = (values * lax.rsqrt(mean + 1e-06)).astype(jnp.bfloat16)

    with jax.named_scope("norm"):
        each(UNITS, lambda u: normalise(raw, unit, u))

    @pl.when(asks)
    def _():
        with jax.named_scope("fhello"):
            pl.semaphore_wait(far_hello, 1)

    @pl.when(sends_far)
    def _():
        each(TILES, lambda t: far_copy(0, t, b - 2 * s).start())

    @pl.when(no_far)
    def _():
        each(TILES, lambda t: far_copy(1, t, b + 2 * s).start())

    def scores(left, right):
        return lax.dot_general(
            left, right, (((1,), (1,)), ((), ())), preferred_element_type=jnp.float32
        )

    def own_unit(u):
        left = unit[tile_rows(u, UNIT), :]
        for n in range(UNITS):
            span = slice(n * UNIT, n * UNIT + UNIT)
            block = scores(left, unit[span, :])
            at = lax.broadcasted_iota(jnp.int32, (UNIT, UNIT), 0) + u * UNIT
            to = lax.broadcasted_iota(jnp.int32, (UNIT, UNIT), 1) + n * UNIT
            block = jnp.where(at == to, -jnp.inf, block)
            for q in range(UNIT // TILE):
                out_ref[pl.ds(16 + 2 * u + q, 1), span] = (
                    jnp.max(block[q * TILE : q * TILE + TILE, :], axis=0, keepdims=True) * scale
                )

    def pair_unit(keys_ref, rows_ref, u, by_row, row_base, by_key, key_base, parts=UNITS):
        left = keys_ref[tile_rows(u, UNIT), :]
        for n in range(parts):
            span = slice(n * UNIT, n * UNIT + UNIT)
            block = scores(left, rows_ref[span, :])
            for q in range(UNIT // TILE):
                part = block[q * TILE : q * TILE + TILE, :]
                by_row[pl.ds(row_base + 2 * u + q, 1), span] = (
                    jnp.max(part, axis=0, keepdims=True) * scale
                )
                columns = pl.ds(pl.multiple_of(u * UNIT + q * TILE, TILE), TILE)
                for h in range(UNIT // TILE):
                    turned = jnp.transpose(part[:, h * TILE : h * TILE + TILE])
                    by_key[pl.ds(key_base + 2 * n + h, 1), columns] = (
                        jnp.max(turned, axis=0, keepdims=True) * scale
                    )

    def slot(offset):
        return pl.multiple_of((offset + 2) * TILES, TILES)

    def take(landing, ref, sems, u):
        rows = tile_rows(u, UNIT)
        pltpu.make_async_copy(raw.at[rows], landing.at[rows], sems.at[u]).wait()
        normalise(landing, ref, u)

    def message(k, block, offset):
        return remote(
            back.at[pl.ds(k * TILES, TILES)],
            out_ref.at[pl.ds(slot(offset), TILES)],
            back_send.at[k],
            back_sem.at[offset + 2],
            block,
        )

    def far_unit(u):
        with jax.named_scope("farw"):
            take(far_in, far, far_sem, u)
        with jax.named_scope("farc"):
            pair_unit(far, unit, u, out_ref, slot(2 * s), back, 0)

    def near_take(u):
        with jax.named_scope("nearw"):
            take(near_in, near, near_sem, u)

    def near_score(u):
        with jax.named_scope("nearc"):
            pair_unit(near, unit, u, out_ref, slot(s), back, TILES)

    def near_unit(u):
        near_take(u)
        near_score(u)

    def near_far_unit(u):
        with jax.named_scope("nfc"):
            pair_unit(near, far, u, back, 2 * TILES, back, 3 * TILES)

    def extra_take(u):
        with jax.named_scope("xw"):
            take(extra_in, extra, extra_sem, u)

    def extra_score(u):
        with jax.named_scope("xuc"):
            pair_unit(extra, unit, u, out_ref, slot(1), back, 4 * TILES)

    def extra_unit(u):
        extra_take(u)
        extra_score(u)

    def extra_near_unit(u, parts=UNITS - 1):
        with jax.named_scope("xnc"):
            pair_unit(extra, near, u, back, 5 * TILES, back, 6 * TILES, parts)

    def last_near_extra(parts=UNITS):
        with jax.named_scope("nxc"):
            pair_unit(near, extra, UNITS - 1, back, 6 * TILES, back, 5 * TILES, parts)

    def seam_forward(t):
        rows = tile_rows(t, PIECE)
        with jax.named_scope("passw"):
            pltpu.make_async_copy(raw.at[rows], pass_on.at[rows], pass_sem.at[t]).wait()
        seam_pass(t, pass_to).start()

    @pl.when(passes)
    def _():
        @pl.when(pass_o)
        def _():
            with jax.named_scope("hello"):
                pl.semaphore_wait(hello, 1)

        each(LEAD, seam_forward)

    def forward(i):
        @pl.when(both(passes, i < (PIECES - LEAD) // 2))
        def _():
            seam_forward(LEAD + 2 * i)
            seam_forward(LEAD + 2 * i + 1)

        @pl.when(i < around)
        def _():
            rows = tile_rows(i, PIECE)
            with jax.named_scope("ringw"):
                pltpu.make_async_copy(raw.at[rows], ring.at[rows], ring_sem.at[i]).wait()

            @pl.when(even)
            def _():
                leg_two(i).start()

            @pl.when(odd)
            def _():
                leg_three(i).start()

        @pl.when(both(slow, odd, i == 8))
        def _():
            each(direct, lambda j: straight(j).start())

        @pl.when(i < UNITS)
        def _():
            with jax.named_scope("own"):
                own_unit(i)

    each(jnp.where(slow, SEAM_AROUND, AROUND + 1), forward)

    plain = both(even, jnp.logical_not(cross_e))

    def extra_take_near(u):
        extra_take(u)
        extra_near_unit(u)

    def arrive(k):
        @pl.when(both(even, step_in, k == 3))
        def _():
            near_unit(2)

        @pl.when(has_far)
        def _():
            far_unit(k)

        @pl.when(both(plain, jnp.logical_not(slow), jnp.logical_or(k == 1, k == 2)))
        def _():
            near_unit(k - 1)

    each(UNITS, arrive)

    @pl.when(has_far)
    def _():
        message(0, b + 2 * s, -2 * s).start()

    @pl.when(plain)
    def _():
        def rest(k):
            @pl.when(jnp.logical_or(both(k == 2, jnp.logical_not(step_in)), both(slow, k < 2)))
            def _():
                near_unit(k)

            @pl.when(both(cross_o, k == 2))
            def _():
                each(2, extra_take_near)

            @pl.when(both(cross_o, k == 3))
            def _():
                extra_take_near(2)

            @pl.when(k == 3)
            def _():
                near_take(3)

            @pl.when(has_far)
            def _():
                near_far_unit(k)

        each(UNITS, rest)

        @pl.when(has_far)
        def _():
            message(2, b + 2 * s, -s).start()
            message(3, mate, s).start()

        near_score(3)
        message(1, mate, -s).start()

        @pl.when(cross_o)
        def _():
            last_near_extra(UNITS - 1)
            extra_take(3)
            extra_near_unit(3, UNITS)
            message(5, mate, -2).start()

    @pl.when(cross_e)
    def _():
        def all_three(u):
            near_unit(u)
            near_far_unit(u)
            extra_unit(u)

        each(UNITS - 1, all_three)
        each(UNITS - 1, extra_near_unit)
        near_take(3)
        extra_take(3)
        extra_near_unit(3)
        last_near_extra()
        message(6, over, -2).start()
        message(5, mate, 2).start()
        extra_score(3)
        message(4, over, -1).start()
        near_far_unit(3)
        message(2, b + 2 * s, -s).start()
        message(3, mate, s).start()
        near_score(3)
        message(1, mate, -s).start()

    @pl.when(cross_o)
    def _():
        pl.semaphore_wait(hello, 1)
        message(6, over, 2).start()

    def landed(offset):
        pltpu.make_async_copy(
            back.at[pl.ds(0, TILES)],
            out_ref.at[pl.ds(slot(offset), TILES)],
            back_sem.at[offset + 2],
        ).wait()

    with jax.named_scope("landed"):
        landed(-2 * s)

        @pl.when(jnp.logical_not(cross_e))
        def _():
            landed(-s)

        @pl.when(odd)
        def _():
            landed(s)

        @pl.when(no_far)
        def _():
            landed(2 * s)

    with jax.named_scope("settle"):
        def left(condition, sem, rows=ROWS):
            @pl.when(condition)
            def _():
                part = pl.ds(0, rows)
                pltpu.make_async_copy(raw.at[part], raw.at[part], sem).wait()

        usual = jnp.logical_not(last_e)
        left(both(usual, low), ring_send, AROUND * PIECE)
        left(both(usual, high), ring_send, (AROUND + 1) * PIECE)
        left(slow, ring_send, SEAM_AROUND * PIECE)
        left(odd, near_send)
        left(sends_far, far_send.at[0])
        left(no_far, far_send.at[1])
        left(cross, extra_send)
        left(passes, pass_send)

        @pl.when(has_far)
        def _():
            message(0, b + 2 * s, -2 * s).wait_send()

        @pl.when(even)
        def _():
            message(1, mate, -s).wait_send()

            @pl.when(has_far)
            def _():
                message(2, b + 2 * s, -s).wait_send()
                message(3, mate, s).wait_send()

        @pl.when(cross_e)
        def _():
            message(4, over, -1).wait_send()

        @pl.when(cross)
        def _():
            message(5, mate, 2 * s).wait_send()
            message(6, over, 2 * s).wait_send()


def body(embeddings):
    rows, width = embeddings.shape
    block = pltpu.VMEM((rows, width), jnp.bfloat16)
    dma = pltpu.SemaphoreType.DMA
    tiles_t = pl.pallas_call(
        kernel,
        name="cycle_tile_max",
        out_shape=jax.ShapeDtypeStruct((5 * TILES, rows), jnp.float32),
        in_specs=[pl.BlockSpec(memory_space=pltpu.HBM)],
        out_specs=pl.BlockSpec(memory_space=pltpu.VMEM),
        scratch_shapes=[
            block,
            block,
            block,
            block,
            block,
            block,
            block,
            block,
            block,
            pltpu.VMEM((SEAM_AROUND * PIECE, width), jnp.bfloat16),
            pltpu.VMEM((7 * TILES, rows), jnp.float32),
            dma,
            dma,
            dma((UNITS,)),
            dma,
            dma((SEAM_AROUND,)),
            dma((2,)),
            dma((UNITS,)),
            dma,
            dma((UNITS,)),
            dma((PIECES,)),
            dma,
            dma((7,)),
            dma((5,)),
            pltpu.SemaphoreType.REGULAR,
            pltpu.SemaphoreType.REGULAR,
        ],
        compiler_params=pltpu.CompilerParams(
            collective_id=0, has_side_effects=True, vmem_limit_bytes=52 * 2**20
        ),
        cost_estimate=pl.CostEstimate(
            flops=8 * 1024**3, bytes_accessed=4 * 2**20, transcendentals=0
        ),
    )(embeddings)
    return jnp.transpose(tiles_t)


def solution(mesh):
    return jax.shard_map(
        body,
        mesh=mesh,
        in_specs=(P(("blk", "grp"), None),),
        out_specs=P(("blk", "grp"), None),
        check_vma=False,
    )
```

```python
import jax
import jax.numpy as jnp
from jax import lax
from jax.experimental import pallas as pl
from jax.experimental.pallas import tpu as pltpu
from jax.sharding import PartitionSpec as P

MESH = pl.DeviceIdType.MESH
ROWS = 1024
TILE = 128
TILES = ROWS // TILE
UNIT = 256
UNITS = ROWS // UNIT
PIECE = 32
PIECES = ROWS // PIECE
AROUND = 10
SEAM_AROUND = 20
LEAD = 8
STEPS = (PIECES - LEAD) // 2
GRP = 2
BLOCKS = 256


def where_of(block):
    block = lax.rem(block + BLOCKS, BLOCKS)
    return (lax.div(block, GRP), lax.rem(block, GRP))


def both(*conditions):
    out = conditions[0]
    for condition in conditions[1:]:
        out = jnp.logical_and(out, condition)
    return out


def kernel(
    x_ref,
    out_ref,
    raw,
    unit,
    near,
    far,
    extra,
    near_in,
    far_in,
    extra_in,
    pass_on,
    ring,
    back,
    load_sem,
    near_send,
    near_sem,
    ring_send,
    ring_sem,
    far_send,
    far_sem,
    extra_send,
    extra_sem,
    pass_sem,
    pass_send,
    back_send,
    back_sem,
    hello,
    far_hello,
):
    b = lax.axis_index("blk") * GRP + lax.axis_index("grp")
    m = lax.rem(b, 4)
    z = lax.rem(lax.div(b, 4), 8)
    x = lax.rem(lax.div(b, 32), 4)
    half = lax.div(b, 128)
    y = half * 2 + lax.rem(b, 2)
    scale = 1.0 / 1024**0.5

    def at_y(offset):
        to = lax.rem(y + offset + 4, 4)
        return lax.div(to, 2) * 128 + lax.rem(b, 128) - lax.rem(b, 2) + lax.rem(to, 2)

    is_e = x >= 1
    s = jnp.where(is_e, -1, 1)
    role = jnp.where(is_e, 3 - m, m)
    even = lax.rem(role, 2) == 0
    odd = jnp.logical_not(even)
    low = m < 2
    high = jnp.logical_not(low)
    first_o = both(x == 0, z == 0)
    last_o = both(x == 0, z == 7)
    last_e = both(x == 3, z == 7)

    mate = b + 1 - 2 * lax.rem(m, 2)
    ahead = at_y(s)
    behind = at_y(-s)
    no_far = both(last_o, high)
    has_far = jnp.logical_not(no_far)
    no_send = jnp.logical_or(both(first_o, low), both(last_e, high))
    sends_far = jnp.logical_not(no_send)
    cross_e = both(last_e, m == 3)
    cross_o = both(first_o, m == 0)
    cross = jnp.logical_or(cross_e, cross_o)
    pass_e = both(last_e, m == 2)
    pass_o = both(first_o, m == 1)
    passes = jnp.logical_or(pass_e, pass_o)
    over = jnp.where(is_e, b + 1, b - 1)
    seam_e = half * 128 + 127
    seam_o = half * 128
    slow = both(last_e, low)
    step_in = both(is_e, z == 0, low)
    step_out = both(is_e, z == 7, high)
    answers = both(is_e, jnp.logical_not(step_in))
    asks = both(is_e, sends_far, jnp.logical_not(step_out))
    around = jnp.where(last_e, jnp.where(low, SEAM_AROUND, 0), jnp.where(low, AROUND, AROUND + 1))
    direct = PIECES - around

    load = pltpu.make_async_copy(x_ref, raw, load_sem)
    load.start()

    barrier = pltpu.get_barrier_semaphore()

    def greet(condition, *blocks):
        def send():
            for block in blocks:
                pl.semaphore_signal(
                    barrier, inc=1, device_id=where_of(block), device_id_type=MESH
                )

        if condition is None:
            send()
        else:
            pl.when(condition)(send)

    greet(None, behind)
    greet(even, mate)
    greet(both(has_far, jnp.logical_not(answers)), b + 2 * s)
    greet(asks, b - 2 * s)
    greet(cross_o, half * 128 + 126, over)
    greet(pass_o, seam_e, at_y(1))
    greet(pass_e, at_y(-1))

    def one(condition):
        return condition.astype(jnp.int32)

    with jax.named_scope("bar"):
        pl.semaphore_wait(
            barrier,
            1
            + one(odd)
            + one(both(sends_far, jnp.logical_not(asks)))
        + one(answers)
            + one(no_far)
            + 3 * one(cross_e)
            + one(pass_e)
            + one(cross_o),
        )

    @pl.when(cross_e)
    def _():
        for block in (over, seam_o + 1):
            pl.semaphore_signal(hello, inc=1, device_id=where_of(block), device_id_type=MESH)

    @pl.when(answers)
    def _():
        pl.semaphore_signal(
            far_hello, inc=1, device_id=where_of(b + 2 * s), device_id_type=MESH
        )

    with jax.named_scope("load"):
        load.wait()

    def tile_rows(t, size):
        return pl.ds(pl.multiple_of(t * size, size), size)

    def around_piece(i):
        fewer = jnp.where(i < 6, i + 18, i + 22)
        more = jnp.where(i < 7, jnp.where(i < 3, 19, i + 17), i + 21)
        usual = jnp.where(i < 2, i + 14, jnp.where(low, fewer, more))
        return jnp.where(slow, i, usual)

    def direct_piece(j):
        fewer = jnp.where(j < 18, j + 2, j + 6)
        more = jnp.where(j < 17, j + 2, j + 7)
        usual = jnp.where(j < 14, j, jnp.where(low, fewer, more))
        return jnp.where(slow, j + SEAM_AROUND, jnp.where(last_e, j, usual))

    def remote(src, dst, send, recv, block):
        return pltpu.make_async_remote_copy(
            src_ref=src,
            dst_ref=dst,
            send_sem=send,
            recv_sem=recv,
            device_id=where_of(block),
            device_id_type=MESH,
        )

    def leg_one(i):
        p = around_piece(i)
        return remote(
            raw.at[tile_rows(p, PIECE)],
            ring.at[tile_rows(i, PIECE)],
            near_send,
            ring_sem.at[i],
            ahead,
        )

    def straight(j):
        p = direct_piece(j)
        rows = tile_rows(p, PIECE)
        return remote(raw.at[rows], near_in.at[rows], near_send, near_sem.at[lax.div(p, UNIT // PIECE)], mate)

    def leg_two(i):
        rows = tile_rows(i, PIECE)
        return remote(ring.at[rows], ring.at[rows], ring_send, ring_sem.at[i], ahead)

    def leg_three(i):
        p = around_piece(i)
        return remote(
            ring.at[tile_rows(i, PIECE)],
            near_in.at[tile_rows(p, PIECE)],
            ring_send,
            near_sem.at[lax.div(p, UNIT // PIECE)],
            ahead,
        )

    def far_copy(which, t, block):
        rows = tile_rows(t, TILE)
        return remote(raw.at[rows], far_in.at[rows], far_send.at[which], far_sem.at[lax.div(t, UNIT // TILE)], block)

    def seam_copy(t, block):
        rows = tile_rows(t, PIECE)
        return remote(raw.at[rows], pass_on.at[rows], extra_send, pass_sem.at[t], block)

    def seam_pass(t, block):
        rows = tile_rows(t, PIECE)
        return remote(pass_on.at[rows], extra_in.at[rows], pass_send, extra_sem.at[lax.div(t, UNIT // PIECE)], block)

    def each(count, body):
        def step(t, carry):
            body(t)
            return carry

        lax.fori_loop(0, count, step, 0)

    seam_to = jnp.where(cross_e, at_y(1), at_y(-1))
    pass_to = jnp.where(pass_e, seam_o, seam_e)

    @pl.when(odd)
    def _():
        each(around, lambda i: leg_one(i).start())

        @pl.when(jnp.logical_not(slow))
        def _():
            each(direct, lambda j: straight(j).start())

    @pl.when(cross)
    def _():
        each(PIECES, lambda t: seam_copy(t, seam_to).start())

    def normalise(src, dst, u):
        for k in range(UNIT // 64):
            rows = pl.ds(pl.multiple_of(u * UNIT + k * 64, 64), 64)
            values = src[rows, :].astype(jnp.float32)
            mean = jnp.mean(values * values, axis=-1, keepdims=True)
            dst[rows, :] = (values * lax.rsqrt(mean + 1e-06)).astype(jnp.bfloat16)

    with jax.named_scope("norm"):
        each(UNITS, lambda u: normalise(raw, unit, u))

    @pl.when(asks)
    def _():
        with jax.named_scope("fhello"):
            pl.semaphore_wait(far_hello, 1)

    @pl.when(sends_far)
    def _():
        each(TILES, lambda t: far_copy(0, t, b - 2 * s).start())

    @pl.when(no_far)
    def _():
        each(TILES, lambda t: far_copy(1, t, b + 2 * s).start())

    def scores(left, right):
        return lax.dot_general(
            left, right, (((1,), (1,)), ((), ())), preferred_element_type=jnp.float32
        )

    def own_unit(u):
        left = unit[tile_rows(u, UNIT), :]
        for n in range(UNITS):
            span = slice(n * UNIT, n * UNIT + UNIT)
            block = scores(left, unit[span, :])
            at = lax.broadcasted_iota(jnp.int32, (UNIT, UNIT), 0) + u * UNIT
            to = lax.broadcasted_iota(jnp.int32, (UNIT, UNIT), 1) + n * UNIT
            block = jnp.where(at == to, -jnp.inf, block)
            for q in range(UNIT // TILE):
                out_ref[pl.ds(16 + 2 * u + q, 1), span] = (
                    jnp.max(block[q * TILE : q * TILE + TILE, :], axis=0, keepdims=True) * scale
                )

    def pair_unit(keys_ref, rows_ref, u, by_row, row_base, by_key, key_base, parts=UNITS, first=0):
        left = keys_ref[tile_rows(u, UNIT), :]
        for n in range(first, parts):
            span = slice(n * UNIT, n * UNIT + UNIT)
            block = scores(left, rows_ref[span, :])
            for q in range(UNIT // TILE):
                part = block[q * TILE : q * TILE + TILE, :]
                by_row[pl.ds(row_base + 2 * u + q, 1), span] = (
                    jnp.max(part, axis=0, keepdims=True) * scale
                )
                columns = pl.ds(pl.multiple_of(u * UNIT + q * TILE, TILE), TILE)
                for h in range(UNIT // TILE):
                    turned = jnp.transpose(part[:, h * TILE : h * TILE + TILE])
                    by_key[pl.ds(key_base + 2 * n + h, 1), columns] = (
                        jnp.max(turned, axis=0, keepdims=True) * scale
                    )

    def slot(offset):
        return pl.multiple_of((offset + 2) * TILES, TILES)

    def take(landing, ref, sems, u):
        rows = tile_rows(u, UNIT)
        pltpu.make_async_copy(raw.at[rows], landing.at[rows], sems.at[u]).wait()
        normalise(landing, ref, u)

    def message(k, block, offset):
        return remote(
            back.at[pl.ds(k * TILES, TILES)],
            out_ref.at[pl.ds(slot(offset), TILES)],
            back_send.at[k],
            back_sem.at[offset + 2],
            block,
        )

    def far_unit(u):
        with jax.named_scope("farw"):
            take(far_in, far, far_sem, u)
        with jax.named_scope("farc"):
            pair_unit(far, unit, u, out_ref, slot(2 * s), back, 0)

    def near_take(u):
        with jax.named_scope("nearw"):
            take(near_in, near, near_sem, u)

    def near_score(u):
        with jax.named_scope("nearc"):
            pair_unit(near, unit, u, out_ref, slot(s), back, TILES)

    def near_unit(u):
        near_take(u)
        near_score(u)

    def near_far_unit(u):
        with jax.named_scope("nfc"):
            pair_unit(near, far, u, back, 2 * TILES, back, 3 * TILES)

    def extra_take(u):
        with jax.named_scope("xw"):
            take(extra_in, extra, extra_sem, u)

    def far_near_unit(u):
        with jax.named_scope("fnc"):
            pair_unit(far, near, u, back, 3 * TILES, back, 2 * TILES, 2)

    def extra_score(u):
        with jax.named_scope("xuc"):
            pair_unit(extra, unit, u, out_ref, slot(1), back, 4 * TILES)

    def extra_unit(u):
        extra_take(u)
        extra_score(u)

    def extra_near_unit(u, parts=UNITS - 1):
        with jax.named_scope("xnc"):
            pair_unit(extra, near, u, back, 5 * TILES, back, 6 * TILES, parts)

    def extra_near_span(u, first, parts):
        with jax.named_scope("xns"):
            pair_unit(extra, near, u, back, 5 * TILES, back, 6 * TILES, parts, first)

    def last_near_extra(parts=UNITS):
        with jax.named_scope("nxc"):
            pair_unit(near, extra, UNITS - 1, back, 6 * TILES, back, 5 * TILES, parts)

    def seam_forward(t):
        rows = tile_rows(t, PIECE)
        with jax.named_scope("passw"):
            pltpu.make_async_copy(raw.at[rows], pass_on.at[rows], pass_sem.at[t]).wait()
        seam_pass(t, pass_to).start()

    @pl.when(passes)
    def _():
        @pl.when(pass_o)
        def _():
            with jax.named_scope("hello"):
                pl.semaphore_wait(hello, 1)

        each(LEAD, seam_forward)

    def forward(i):
        @pl.when(both(passes, i < STEPS))
        def _():
            seam_forward(LEAD + 2 * i)
            seam_forward(LEAD + 2 * i + 1)

        @pl.when(i < around)
        def _():
            rows = tile_rows(i, PIECE)
            with jax.named_scope("ringw"):
                pltpu.make_async_copy(raw.at[rows], ring.at[rows], ring_sem.at[i]).wait()

            @pl.when(even)
            def _():
                leg_two(i).start()

            @pl.when(odd)
            def _():
                leg_three(i).start()

        @pl.when(both(slow, odd, i == 16))
        def _():
            each(direct, lambda j: straight(j).start())

        @pl.when(i < UNITS)
        def _():
            with jax.named_scope("own"):
                own_unit(i)

    each(jnp.where(slow, SEAM_AROUND, STEPS), forward)

    plain = both(even, jnp.logical_not(cross_e))

    def arrive(k):
        @pl.when(both(even, step_in, k == 2))
        def _():
            near_unit(1)

        @pl.when(both(even, step_in, k == 3))
        def _():
            each(3, far_near_unit)
            near_unit(2)

        @pl.when(has_far)
        def _():
            far_unit(k)

        @pl.when(both(even, step_in, k == 3))
        def _():
            far_near_unit(3)

        @pl.when(
            both(
                plain,
                jnp.logical_not(slow),
                jnp.logical_or(k == 1, both(k == 2, jnp.logical_not(step_in))),
            )
        )
        def _():
            near_unit(k - 1)

    each(UNITS, arrive)

    @pl.when(has_far)
    def _():
        message(0, b + 2 * s, -2 * s).start()

    @pl.when(plain)
    def _():
        def rest(k):
            @pl.when(both(cross_o, k == 2))
            def _():
                each(2, extra_take)
                each(2, lambda u: extra_near_unit(u, 2))

            @pl.when(jnp.logical_or(both(k == 2, jnp.logical_not(step_in)), both(slow, k < 2)))
            def _():
                near_unit(k)

            @pl.when(both(cross_o, k == 2))
            def _():
                each(2, lambda u: extra_near_span(u, 2, UNITS - 1))

            @pl.when(both(cross_o, k == 3))
            def _():
                extra_take(2)
                extra_near_unit(2)

            @pl.when(k == 3)
            def _():
                near_take(3)

            @pl.when(both(has_far, jnp.logical_or(k >= 2, jnp.logical_not(step_in))))
            def _():
                near_far_unit(k)

        each(UNITS, rest)

        @pl.when(has_far)
        def _():
            message(2, b + 2 * s, -s).start()
            message(3, mate, s).start()

        near_score(3)
        message(1, mate, -s).start()

        @pl.when(cross_o)
        def _():
            last_near_extra(UNITS - 1)
            extra_take(3)
            extra_near_unit(3, UNITS)
            message(5, mate, -2).start()

    @pl.when(cross_e)
    def _():
        def all_three(u):
            near_unit(u)
            near_far_unit(u)
            extra_unit(u)

        each(UNITS - 1, all_three)
        each(UNITS - 1, extra_near_unit)
        near_take(3)
        last_near_extra(UNITS - 1)
        extra_take(3)
        extra_near_unit(3, UNITS)
        message(6, over, -2).start()
        message(5, mate, 2).start()
        extra_score(3)
        message(4, over, -1).start()
        near_far_unit(3)
        message(2, b + 2 * s, -s).start()
        message(3, mate, s).start()
        near_score(3)
        message(1, mate, -s).start()

    @pl.when(cross_o)
    def _():
        pl.semaphore_wait(hello, 1)
        message(6, over, 2).start()

    def landed(offset):
        pltpu.make_async_copy(
            back.at[pl.ds(0, TILES)],
            out_ref.at[pl.ds(slot(offset), TILES)],
            back_sem.at[offset + 2],
        ).wait()

    with jax.named_scope("landed"):
        landed(-2 * s)

        @pl.when(jnp.logical_not(cross_e))
        def _():
            landed(-s)

        @pl.when(odd)
        def _():
            landed(s)

        @pl.when(no_far)
        def _():
            landed(2 * s)

    with jax.named_scope("settle"):
        def left(condition, sem, rows=ROWS):
            @pl.when(condition)
            def _():
                part = pl.ds(0, rows)
                pltpu.make_async_copy(raw.at[part], raw.at[part], sem).wait()

        usual = jnp.logical_not(last_e)
        left(both(usual, low), ring_send, AROUND * PIECE)
        left(both(usual, high), ring_send, (AROUND + 1) * PIECE)
        left(slow, ring_send, SEAM_AROUND * PIECE)
        left(odd, near_send)
        left(sends_far, far_send.at[0])
        left(no_far, far_send.at[1])
        left(cross, extra_send)
        left(passes, pass_send)

        @pl.when(has_far)
        def _():
            message(0, b + 2 * s, -2 * s).wait_send()

        @pl.when(even)
        def _():
            message(1, mate, -s).wait_send()

            @pl.when(has_far)
            def _():
                message(2, b + 2 * s, -s).wait_send()
                message(3, mate, s).wait_send()

        @pl.when(cross_e)
        def _():
            message(4, over, -1).wait_send()

        @pl.when(cross)
        def _():
            message(5, mate, 2 * s).wait_send()
            message(6, over, 2 * s).wait_send()


def body(embeddings):
    rows, width = embeddings.shape
    block = pltpu.VMEM((rows, width), jnp.bfloat16)
    dma = pltpu.SemaphoreType.DMA
    tiles_t = pl.pallas_call(
        kernel,
        name="cycle_tile_max",
        out_shape=jax.ShapeDtypeStruct((5 * TILES, rows), jnp.float32),
        in_specs=[pl.BlockSpec(memory_space=pltpu.HBM)],
        out_specs=pl.BlockSpec(memory_space=pltpu.VMEM),
        scratch_shapes=[
            block,
            block,
            block,
            block,
            block,
            block,
            block,
            block,
            block,
            pltpu.VMEM((SEAM_AROUND * PIECE, width), jnp.bfloat16),
            pltpu.VMEM((7 * TILES, rows), jnp.float32),
            dma,
            dma,
            dma((UNITS,)),
            dma,
            dma((SEAM_AROUND,)),
            dma((2,)),
            dma((UNITS,)),
            dma,
            dma((UNITS,)),
            dma((PIECES,)),
            dma,
            dma((7,)),
            dma((5,)),
            pltpu.SemaphoreType.REGULAR,
            pltpu.SemaphoreType.REGULAR,
        ],
        compiler_params=pltpu.CompilerParams(
            collective_id=0, has_side_effects=True, vmem_limit_bytes=52 * 2**20
        ),
        cost_estimate=pl.CostEstimate(
            flops=8 * 1024**3, bytes_accessed=4 * 2**20, transcendentals=0
        ),
    )(embeddings)
    return jnp.transpose(tiles_t)


def solution(mesh):
    return jax.shard_map(
        body,
        mesh=mesh,
        in_specs=(P(("blk", "grp"), None),),
        out_specs=P(("blk", "grp"), None),
        check_vma=False,
    )
```

```python
import jax
import jax.numpy as jnp
from jax import lax
from jax.experimental import pallas as pl
from jax.experimental.pallas import tpu as pltpu
from jax.sharding import PartitionSpec as P

MESH = pl.DeviceIdType.MESH
ROWS = 1024
TILE = 128
TILES = ROWS // TILE
UNIT = 256
UNITS = ROWS // UNIT
PIECE = 32
PIECES = ROWS // PIECE
AROUND = 10
SEAM_AROUND = 20
LEAD = 8
STEPS = (PIECES - LEAD) // 2
GRP = 2
BLOCKS = 256


def where_of(block):
    block = lax.rem(block + BLOCKS, BLOCKS)
    return (lax.div(block, GRP), lax.rem(block, GRP))


def both(*conditions):
    out = conditions[0]
    for condition in conditions[1:]:
        out = jnp.logical_and(out, condition)
    return out


def kernel(
    x_ref,
    out_ref,
    raw,
    unit,
    near,
    far,
    extra,
    near_in,
    far_in,
    extra_in,
    pass_on,
    ring,
    back,
    load_sem,
    near_send,
    near_sem,
    ring_send,
    ring_sem,
    far_send,
    far_sem,
    extra_send,
    extra_sem,
    pass_sem,
    pass_send,
    back_send,
    back_sem,
    hello,
    far_hello,
):
    b = lax.axis_index("blk") * GRP + lax.axis_index("grp")
    m = lax.rem(b, 4)
    z = lax.rem(lax.div(b, 4), 8)
    x = lax.rem(lax.div(b, 32), 4)
    half = lax.div(b, 128)
    y = half * 2 + lax.rem(b, 2)
    scale = 1.0 / 1024**0.5

    def at_y(offset):
        to = lax.rem(y + offset + 4, 4)
        return lax.div(to, 2) * 128 + lax.rem(b, 128) - lax.rem(b, 2) + lax.rem(to, 2)

    is_e = x >= 1
    s = jnp.where(is_e, -1, 1)
    role = jnp.where(is_e, 3 - m, m)
    even = lax.rem(role, 2) == 0
    odd = jnp.logical_not(even)
    low = m < 2
    high = jnp.logical_not(low)
    first_o = both(x == 0, z == 0)
    last_o = both(x == 0, z == 7)
    last_e = both(x == 3, z == 7)

    mate = b + 1 - 2 * lax.rem(m, 2)
    ahead = at_y(s)
    behind = at_y(-s)
    no_far = both(last_o, high)
    has_far = jnp.logical_not(no_far)
    no_send = jnp.logical_or(both(first_o, low), both(last_e, high))
    sends_far = jnp.logical_not(no_send)
    cross_e = both(last_e, m == 3)
    cross_o = both(first_o, m == 0)
    cross = jnp.logical_or(cross_e, cross_o)
    pass_e = both(last_e, m == 2)
    pass_o = both(first_o, m == 1)
    passes = jnp.logical_or(pass_e, pass_o)
    over = jnp.where(is_e, b + 1, b - 1)
    seam_e = half * 128 + 127
    seam_o = half * 128
    slow = both(last_e, low)
    step_in = both(is_e, z == 0, low)
    step_out = both(is_e, z == 7, high)
    answers = both(is_e, jnp.logical_not(step_in))
    asks = both(is_e, sends_far, jnp.logical_not(step_out))
    around = jnp.where(last_e, jnp.where(low, SEAM_AROUND, 0), jnp.where(low, AROUND, AROUND + 1))
    direct = PIECES - around

    load = pltpu.make_async_copy(x_ref, raw, load_sem)
    load.start()

    barrier = pltpu.get_barrier_semaphore()

    def greet(condition, *blocks):
        def send():
            for block in blocks:
                pl.semaphore_signal(
                    barrier, inc=1, device_id=where_of(block), device_id_type=MESH
                )

        if condition is None:
            send()
        else:
            pl.when(condition)(send)

    greet(None, behind)
    greet(even, mate)
    greet(both(has_far, jnp.logical_not(answers)), b + 2 * s)
    greet(asks, b - 2 * s)
    greet(cross_o, half * 128 + 126, over)
    greet(pass_o, seam_e, at_y(1))
    greet(pass_e, at_y(-1))

    def one(condition):
        return condition.astype(jnp.int32)

    with jax.named_scope("bar"):
        pl.semaphore_wait(
            barrier,
            1
            + one(odd)
            + one(both(sends_far, jnp.logical_not(asks)))
        + one(answers)
            + one(no_far)
            + 3 * one(cross_e)
            + one(pass_e)
            + one(cross_o),
        )

    @pl.when(cross_e)
    def _():
        for block in (over, seam_o + 1):
            pl.semaphore_signal(hello, inc=1, device_id=where_of(block), device_id_type=MESH)

    @pl.when(answers)
    def _():
        pl.semaphore_signal(
            far_hello, inc=1, device_id=where_of(b + 2 * s), device_id_type=MESH
        )

    with jax.named_scope("load"):
        load.wait()

    def tile_rows(t, size):
        return pl.ds(pl.multiple_of(t * size, size), size)

    def around_piece(i):
        fewer = jnp.where(i < 6, i + 18, i + 22)
        more = jnp.where(i < 7, jnp.where(i < 3, 19, i + 17), i + 21)
        usual = jnp.where(i < 2, i + 14, jnp.where(low, fewer, more))
        return jnp.where(slow, i, usual)

    def direct_piece(j):
        fewer = jnp.where(j < 18, j + 2, j + 6)
        more = jnp.where(j < 17, j + 2, j + 7)
        usual = jnp.where(j < 14, j, jnp.where(low, fewer, more))
        return jnp.where(slow, j + SEAM_AROUND, jnp.where(last_e, j, usual))

    def remote(src, dst, send, recv, block):
        return pltpu.make_async_remote_copy(
            src_ref=src,
            dst_ref=dst,
            send_sem=send,
            recv_sem=recv,
            device_id=where_of(block),
            device_id_type=MESH,
        )

    def leg_one(i):
        p = around_piece(i)
        return remote(
            raw.at[tile_rows(p, PIECE)],
            ring.at[tile_rows(i, PIECE)],
            near_send,
            ring_sem.at[i],
            ahead,
        )

    def straight(j):
        p = direct_piece(j)
        rows = tile_rows(p, PIECE)
        return remote(raw.at[rows], near_in.at[rows], near_send, near_sem.at[lax.div(p, UNIT // PIECE)], mate)

    def leg_two(i):
        rows = tile_rows(i, PIECE)
        return remote(ring.at[rows], ring.at[rows], ring_send, ring_sem.at[i], ahead)

    def leg_three(i):
        p = around_piece(i)
        return remote(
            ring.at[tile_rows(i, PIECE)],
            near_in.at[tile_rows(p, PIECE)],
            ring_send,
            near_sem.at[lax.div(p, UNIT // PIECE)],
            ahead,
        )

    def far_copy(which, t, block):
        rows = tile_rows(t, TILE)
        return remote(raw.at[rows], far_in.at[rows], far_send.at[which], far_sem.at[lax.div(t, UNIT // TILE)], block)

    def seam_copy(t, block):
        rows = tile_rows(t, PIECE)
        return remote(raw.at[rows], pass_on.at[rows], extra_send, pass_sem.at[t], block)

    def seam_pass(t, block):
        rows = tile_rows(t, PIECE)
        return remote(pass_on.at[rows], extra_in.at[rows], pass_send, extra_sem.at[lax.div(t, UNIT // PIECE)], block)

    def each(count, body):
        def step(t, carry):
            body(t)
            return carry

        lax.fori_loop(0, count, step, 0)

    seam_to = jnp.where(cross_e, at_y(1), at_y(-1))
    pass_to = jnp.where(pass_e, seam_o, seam_e)

    @pl.when(odd)
    def _():
        each(around, lambda i: leg_one(i).start())

        @pl.when(jnp.logical_not(slow))
        def _():
            each(direct, lambda j: straight(j).start())

    @pl.when(cross)
    def _():
        each(PIECES, lambda t: seam_copy(t, seam_to).start())

    def normalise(src, dst, u):
        for k in range(UNIT // 64):
            rows = pl.ds(pl.multiple_of(u * UNIT + k * 64, 64), 64)
            values = src[rows, :].astype(jnp.float32)
            mean = jnp.mean(values * values, axis=-1, keepdims=True)
            dst[rows, :] = (values * lax.rsqrt(mean + 1e-06)).astype(jnp.bfloat16)

    with jax.named_scope("norm"):
        each(UNITS, lambda u: normalise(raw, unit, u))

    @pl.when(asks)
    def _():
        with jax.named_scope("fhello"):
            pl.semaphore_wait(far_hello, 1)

    @pl.when(sends_far)
    def _():
        each(TILES, lambda t: far_copy(0, t, b - 2 * s).start())

    @pl.when(no_far)
    def _():
        each(TILES, lambda t: far_copy(1, t, b + 2 * s).start())

    def scores(left, right):
        return lax.dot_general(
            left, right, (((1,), (1,)), ((), ())), preferred_element_type=jnp.float32
        )

    def own_unit(u):
        left = unit[tile_rows(u, UNIT), :]
        for n in range(UNITS):
            span = slice(n * UNIT, n * UNIT + UNIT)
            block = scores(left, unit[span, :])
            at = lax.broadcasted_iota(jnp.int32, (UNIT, UNIT), 0) + u * UNIT
            to = lax.broadcasted_iota(jnp.int32, (UNIT, UNIT), 1) + n * UNIT
            block = jnp.where(at == to, -jnp.inf, block)
            for q in range(UNIT // TILE):
                out_ref[pl.ds(16 + 2 * u + q, 1), span] = (
                    jnp.max(block[q * TILE : q * TILE + TILE, :], axis=0, keepdims=True) * scale
                )

    def pair_unit(keys_ref, rows_ref, u, by_row, row_base, by_key, key_base, parts=UNITS, first=0):
        left = keys_ref[tile_rows(u, UNIT), :]
        for n in range(first, parts):
            span = slice(n * UNIT, n * UNIT + UNIT)
            block = scores(left, rows_ref[span, :])
            for q in range(UNIT // TILE):
                part = block[q * TILE : q * TILE + TILE, :]
                by_row[pl.ds(row_base + 2 * u + q, 1), span] = (
                    jnp.max(part, axis=0, keepdims=True) * scale
                )
                columns = pl.ds(pl.multiple_of(u * UNIT + q * TILE, TILE), TILE)
                for h in range(UNIT // TILE):
                    turned = jnp.transpose(part[:, h * TILE : h * TILE + TILE])
                    by_key[pl.ds(key_base + 2 * n + h, 1), columns] = (
                        jnp.max(turned, axis=0, keepdims=True) * scale
                    )

    def slot(offset):
        return pl.multiple_of((offset + 2) * TILES, TILES)

    def take(landing, ref, sems, u):
        rows = tile_rows(u, UNIT)
        pltpu.make_async_copy(raw.at[rows], landing.at[rows], sems.at[u]).wait()
        normalise(landing, ref, u)

    def message(k, block, offset):
        return remote(
            back.at[pl.ds(k * TILES, TILES)],
            out_ref.at[pl.ds(slot(offset), TILES)],
            back_send.at[k],
            back_sem.at[offset + 2],
            block,
        )

    def far_unit(u):
        with jax.named_scope("farw"):
            take(far_in, far, far_sem, u)
        with jax.named_scope("farc"):
            pair_unit(far, unit, u, out_ref, slot(2 * s), back, 0)

    def near_take(u):
        with jax.named_scope("nearw"):
            take(near_in, near, near_sem, u)

    def near_score(u):
        with jax.named_scope("nearc"):
            pair_unit(near, unit, u, out_ref, slot(s), back, TILES)

    def near_unit(u):
        near_take(u)
        near_score(u)

    def near_far_unit(u):
        with jax.named_scope("nfc"):
            pair_unit(near, far, u, back, 2 * TILES, back, 3 * TILES)

    def extra_take(u):
        with jax.named_scope("xw"):
            take(extra_in, extra, extra_sem, u)

    def far_near_unit(u):
        with jax.named_scope("fnc"):
            pair_unit(far, near, u, back, 3 * TILES, back, 2 * TILES, 2)

    def extra_score(u):
        with jax.named_scope("xuc"):
            pair_unit(extra, unit, u, out_ref, slot(1), back, 4 * TILES)

    def extra_unit(u):
        extra_take(u)
        extra_score(u)

    def extra_near_unit(u, parts=UNITS - 1):
        with jax.named_scope("xnc"):
            pair_unit(extra, near, u, back, 5 * TILES, back, 6 * TILES, parts)

    def extra_near_span(u, first, parts):
        with jax.named_scope("xns"):
            pair_unit(extra, near, u, back, 5 * TILES, back, 6 * TILES, parts, first)

    def last_near_extra(parts=UNITS):
        with jax.named_scope("nxc"):
            pair_unit(near, extra, UNITS - 1, back, 6 * TILES, back, 5 * TILES, parts)

    def seam_forward(t):
        rows = tile_rows(t, PIECE)
        with jax.named_scope("passw"):
            pltpu.make_async_copy(raw.at[rows], pass_on.at[rows], pass_sem.at[t]).wait()
        seam_pass(t, pass_to).start()

    @pl.when(passes)
    def _():
        @pl.when(pass_o)
        def _():
            with jax.named_scope("hello"):
                pl.semaphore_wait(hello, 1)

        each(LEAD, seam_forward)

    def forward(i):
        @pl.when(both(passes, i < STEPS))
        def _():
            seam_forward(LEAD + 2 * i)
            seam_forward(LEAD + 2 * i + 1)

        @pl.when(i < around)
        def _():
            rows = tile_rows(i, PIECE)
            with jax.named_scope("ringw"):
                pltpu.make_async_copy(raw.at[rows], ring.at[rows], ring_sem.at[i]).wait()

            @pl.when(even)
            def _():
                leg_two(i).start()

            @pl.when(odd)
            def _():
                leg_three(i).start()

        @pl.when(both(slow, odd, i == 18))
        def _():
            each(direct, lambda j: straight(j).start())

        @pl.when(i < UNITS)
        def _():
            with jax.named_scope("own"):
                own_unit(i)

    each(jnp.where(slow, SEAM_AROUND, STEPS), forward)

    plain = both(even, jnp.logical_not(cross_e))

    def arrive(k):
        @pl.when(both(even, step_in, k == 2))
        def _():
            near_unit(1)

        @pl.when(both(even, step_in, k == 3))
        def _():
            each(3, far_near_unit)
            near_unit(2)

        @pl.when(has_far)
        def _():
            far_unit(k)

        @pl.when(both(even, step_in, k == 3))
        def _():
            far_near_unit(3)

        @pl.when(
            both(
                plain,
                jnp.logical_not(slow),
                jnp.logical_or(k == 1, both(k == 2, jnp.logical_not(step_in))),
            )
        )
        def _():
            near_unit(k - 1)

    each(UNITS, arrive)

    @pl.when(has_far)
    def _():
        message(0, b + 2 * s, -2 * s).start()

    @pl.when(plain)
    def _():
        def rest(k):
            @pl.when(both(cross_o, k == 2))
            def _():
                each(2, extra_take)
                each(2, lambda u: extra_near_unit(u, 2))

            @pl.when(jnp.logical_or(both(k == 2, jnp.logical_not(step_in)), both(slow, k < 2)))
            def _():
                near_unit(k)

            @pl.when(both(cross_o, k == 2))
            def _():
                each(2, lambda u: extra_near_span(u, 2, UNITS - 1))

            @pl.when(both(cross_o, k == 3))
            def _():
                extra_take(2)
                extra_near_unit(2)

            @pl.when(k == 3)
            def _():
                near_take(3)

            @pl.when(both(has_far, jnp.logical_or(k >= 2, jnp.logical_not(step_in))))
            def _():
                near_far_unit(k)

        each(UNITS, rest)

        @pl.when(has_far)
        def _():
            message(2, b + 2 * s, -s).start()
            message(3, mate, s).start()

        near_score(3)
        message(1, mate, -s).start()

        @pl.when(cross_o)
        def _():
            last_near_extra(UNITS - 1)
            extra_take(3)
            extra_near_unit(3, UNITS)
            message(5, mate, -2).start()

    @pl.when(cross_e)
    def _():
        def all_three(u):
            near_unit(u)
            near_far_unit(u)
            extra_unit(u)

        each(UNITS - 1, all_three)
        each(UNITS - 1, extra_near_unit)
        near_take(3)
        last_near_extra(UNITS - 1)
        extra_take(3)
        extra_near_unit(3, UNITS)
        message(6, over, -2).start()
        message(5, mate, 2).start()
        extra_score(3)
        message(4, over, -1).start()
        near_far_unit(3)
        message(2, b + 2 * s, -s).start()
        message(3, mate, s).start()
        near_score(3)
        message(1, mate, -s).start()

    @pl.when(cross_o)
    def _():
        pl.semaphore_wait(hello, 1)
        message(6, over, 2).start()

    def landed(offset):
        pltpu.make_async_copy(
            back.at[pl.ds(0, TILES)],
            out_ref.at[pl.ds(slot(offset), TILES)],
            back_sem.at[offset + 2],
        ).wait()

    with jax.named_scope("landed"):
        landed(-2 * s)

        @pl.when(jnp.logical_not(cross_e))
        def _():
            landed(-s)

        @pl.when(odd)
        def _():
            landed(s)

        @pl.when(no_far)
        def _():
            landed(2 * s)

    with jax.named_scope("settle"):
        def left(condition, sem, rows=ROWS):
            @pl.when(condition)
            def _():
                part = pl.ds(0, rows)
                pltpu.make_async_copy(raw.at[part], raw.at[part], sem).wait()

        usual = jnp.logical_not(last_e)
        left(both(usual, low), ring_send, AROUND * PIECE)
        left(both(usual, high), ring_send, (AROUND + 1) * PIECE)
        left(slow, ring_send, SEAM_AROUND * PIECE)
        left(odd, near_send)
        left(sends_far, far_send.at[0])
        left(no_far, far_send.at[1])
        left(cross, extra_send)
        left(passes, pass_send)

        @pl.when(has_far)
        def _():
            message(0, b + 2 * s, -2 * s).wait_send()

        @pl.when(even)
        def _():
            message(1, mate, -s).wait_send()

            @pl.when(has_far)
            def _():
                message(2, b + 2 * s, -s).wait_send()
                message(3, mate, s).wait_send()

        @pl.when(cross_e)
        def _():
            message(4, over, -1).wait_send()

        @pl.when(cross)
        def _():
            message(5, mate, 2 * s).wait_send()
            message(6, over, 2 * s).wait_send()


def body(embeddings):
    rows, width = embeddings.shape
    block = pltpu.VMEM((rows, width), jnp.bfloat16)
    dma = pltpu.SemaphoreType.DMA
    tiles_t = pl.pallas_call(
        kernel,
        name="cycle_tile_max",
        out_shape=jax.ShapeDtypeStruct((5 * TILES, rows), jnp.float32),
        in_specs=[pl.BlockSpec(memory_space=pltpu.HBM)],
        out_specs=pl.BlockSpec(memory_space=pltpu.VMEM),
        scratch_shapes=[
            block,
            block,
            block,
            block,
            block,
            block,
            block,
            block,
            block,
            pltpu.VMEM((SEAM_AROUND * PIECE, width), jnp.bfloat16),
            pltpu.VMEM((7 * TILES, rows), jnp.float32),
            dma,
            dma,
            dma((UNITS,)),
            dma,
            dma((SEAM_AROUND,)),
            dma((2,)),
            dma((UNITS,)),
            dma,
            dma((UNITS,)),
            dma((PIECES,)),
            dma,
            dma((7,)),
            dma((5,)),
            pltpu.SemaphoreType.REGULAR,
            pltpu.SemaphoreType.REGULAR,
        ],
        compiler_params=pltpu.CompilerParams(
            collective_id=0, has_side_effects=True, vmem_limit_bytes=52 * 2**20
        ),
        cost_estimate=pl.CostEstimate(
            flops=8 * 1024**3, bytes_accessed=4 * 2**20, transcendentals=0
        ),
    )(embeddings)
    return jnp.transpose(tiles_t)


def solution(mesh):
    return jax.shard_map(
        body,
        mesh=mesh,
        in_specs=(P(("blk", "grp"), None),),
        out_specs=P(("blk", "grp"), None),
        check_vma=False,
    )
```

```python
import jax
import jax.numpy as jnp
from jax import lax
from jax.experimental import pallas as pl
from jax.experimental.pallas import tpu as pltpu
from jax.sharding import PartitionSpec as P

MESH = pl.DeviceIdType.MESH
ROWS = 1024
TILE = 128
TILES = ROWS // TILE
UNIT = 256
UNITS = ROWS // UNIT
PIECE = 32
PIECES = ROWS // PIECE
AROUND = 10
SEAM_AROUND = 20
LEAD = 8
STEPS = (PIECES - LEAD) // 2
GRP = 2
BLOCKS = 256


def where_of(block):
    block = lax.rem(block + BLOCKS, BLOCKS)
    return (lax.div(block, GRP), lax.rem(block, GRP))


def both(*conditions):
    out = conditions[0]
    for condition in conditions[1:]:
        out = jnp.logical_and(out, condition)
    return out


def kernel(
    x_ref,
    out_ref,
    raw,
    unit,
    near,
    far,
    extra,
    near_in,
    far_in,
    extra_in,
    pass_on,
    ring,
    back,
    load_sem,
    near_send,
    near_sem,
    ring_send,
    ring_sem,
    far_send,
    far_sem,
    extra_send,
    extra_sem,
    pass_sem,
    pass_send,
    back_send,
    back_sem,
    hello,
    far_hello,
):
    b = lax.axis_index("blk") * GRP + lax.axis_index("grp")
    m = lax.rem(b, 4)
    z = lax.rem(lax.div(b, 4), 8)
    x = lax.rem(lax.div(b, 32), 4)
    half = lax.div(b, 128)
    y = half * 2 + lax.rem(b, 2)
    scale = 1.0 / 1024**0.5

    def at_y(offset):
        to = lax.rem(y + offset + 4, 4)
        return lax.div(to, 2) * 128 + lax.rem(b, 128) - lax.rem(b, 2) + lax.rem(to, 2)

    is_e = x >= 1
    s = jnp.where(is_e, -1, 1)
    role = jnp.where(is_e, 3 - m, m)
    even = lax.rem(role, 2) == 0
    odd = jnp.logical_not(even)
    low = m < 2
    high = jnp.logical_not(low)
    first_o = both(x == 0, z == 0)
    last_o = both(x == 0, z == 7)
    last_e = both(x == 3, z == 7)

    mate = b + 1 - 2 * lax.rem(m, 2)
    ahead = at_y(s)
    behind = at_y(-s)
    no_far = both(last_o, high)
    has_far = jnp.logical_not(no_far)
    no_send = jnp.logical_or(both(first_o, low), both(last_e, high))
    sends_far = jnp.logical_not(no_send)
    cross_e = both(last_e, m == 3)
    cross_o = both(first_o, m == 0)
    cross = jnp.logical_or(cross_e, cross_o)
    pass_e = both(last_e, m == 2)
    pass_o = both(first_o, m == 1)
    passes = jnp.logical_or(pass_e, pass_o)
    over = jnp.where(is_e, b + 1, b - 1)
    seam_e = half * 128 + 127
    seam_o = half * 128
    slow = both(last_e, low)
    step_in = both(is_e, z == 0, low)
    step_out = both(is_e, z == 7, high)
    answers = both(is_e, jnp.logical_not(step_in))
    asks = both(is_e, sends_far, jnp.logical_not(step_out))
    around = jnp.where(last_e, jnp.where(low, SEAM_AROUND, 0), jnp.where(low, AROUND, AROUND + 1))
    direct = PIECES - around

    load = pltpu.make_async_copy(x_ref, raw, load_sem)
    load.start()

    barrier = pltpu.get_barrier_semaphore()

    def greet(condition, *blocks):
        def send():
            for block in blocks:
                pl.semaphore_signal(
                    barrier, inc=1, device_id=where_of(block), device_id_type=MESH
                )

        if condition is None:
            send()
        else:
            pl.when(condition)(send)

    greet(None, behind)
    greet(even, mate)
    greet(both(has_far, jnp.logical_not(answers)), b + 2 * s)
    greet(asks, b - 2 * s)
    greet(cross_o, half * 128 + 126, over)
    greet(pass_o, seam_e, at_y(1))
    greet(pass_e, at_y(-1))

    def one(condition):
        return condition.astype(jnp.int32)

    with jax.named_scope("bar"):
        pl.semaphore_wait(
            barrier,
            1
            + one(odd)
            + one(both(sends_far, jnp.logical_not(asks)))
        + one(answers)
            + one(no_far)
            + 3 * one(cross_e)
            + one(pass_e)
            + one(cross_o),
        )

    @pl.when(cross_e)
    def _():
        for block in (over, seam_o + 1):
            pl.semaphore_signal(hello, inc=1, device_id=where_of(block), device_id_type=MESH)

    @pl.when(answers)
    def _():
        pl.semaphore_signal(
            far_hello, inc=1, device_id=where_of(b + 2 * s), device_id_type=MESH
        )

    with jax.named_scope("load"):
        load.wait()

    def tile_rows(t, size):
        return pl.ds(pl.multiple_of(t * size, size), size)

    def around_piece(i):
        fewer = jnp.where(i < 6, i + 18, i + 22)
        more = jnp.where(i < 7, jnp.where(i < 3, 19, i + 17), i + 21)
        usual = jnp.where(i < 2, i + 14, jnp.where(low, fewer, more))
        return jnp.where(slow, i, usual)

    def direct_piece(j):
        fewer = jnp.where(j < 18, j + 2, j + 6)
        more = jnp.where(j < 17, j + 2, j + 7)
        usual = jnp.where(j < 14, j, jnp.where(low, fewer, more))
        return jnp.where(slow, j + SEAM_AROUND, jnp.where(last_e, j, usual))

    def remote(src, dst, send, recv, block):
        return pltpu.make_async_remote_copy(
            src_ref=src,
            dst_ref=dst,
            send_sem=send,
            recv_sem=recv,
            device_id=where_of(block),
            device_id_type=MESH,
        )

    def leg_one(i):
        p = around_piece(i)
        return remote(
            raw.at[tile_rows(p, PIECE)],
            ring.at[tile_rows(i, PIECE)],
            near_send,
            ring_sem.at[i],
            ahead,
        )

    def straight(j):
        p = direct_piece(j)
        rows = tile_rows(p, PIECE)
        return remote(raw.at[rows], near_in.at[rows], near_send, near_sem.at[lax.div(p, UNIT // PIECE)], mate)

    def leg_two(i):
        rows = tile_rows(i, PIECE)
        return remote(ring.at[rows], ring.at[rows], ring_send, ring_sem.at[i], ahead)

    def leg_three(i):
        p = around_piece(i)
        return remote(
            ring.at[tile_rows(i, PIECE)],
            near_in.at[tile_rows(p, PIECE)],
            ring_send,
            near_sem.at[lax.div(p, UNIT // PIECE)],
            ahead,
        )

    def far_copy(which, t, block):
        rows = tile_rows(t, TILE)
        return remote(raw.at[rows], far_in.at[rows], far_send.at[which], far_sem.at[lax.div(t, UNIT // TILE)], block)

    def seam_copy(t, block):
        rows = tile_rows(t, PIECE)
        return remote(raw.at[rows], pass_on.at[rows], extra_send, pass_sem.at[t], block)

    def seam_pass(t, block):
        rows = tile_rows(t, PIECE)
        return remote(pass_on.at[rows], extra_in.at[rows], pass_send, extra_sem.at[lax.div(t, UNIT // PIECE)], block)

    def each(count, body):
        def step(t, carry):
            body(t)
            return carry

        lax.fori_loop(0, count, step, 0)

    seam_to = jnp.where(cross_e, at_y(1), at_y(-1))
    pass_to = jnp.where(pass_e, seam_o, seam_e)

    @pl.when(odd)
    def _():
        each(around, lambda i: leg_one(i).start())

        @pl.when(jnp.logical_not(slow))
        def _():
            each(direct, lambda j: straight(j).start())

    @pl.when(cross)
    def _():
        each(PIECES, lambda t: seam_copy(t, seam_to).start())

    def normalise(src, dst, u):
        for k in range(UNIT // 64):
            rows = pl.ds(pl.multiple_of(u * UNIT + k * 64, 64), 64)
            values = src[rows, :].astype(jnp.float32)
            mean = jnp.mean(values * values, axis=-1, keepdims=True)
            dst[rows, :] = (values * lax.rsqrt(mean + 1e-06)).astype(jnp.bfloat16)

    with jax.named_scope("norm"):
        each(UNITS, lambda u: normalise(raw, unit, u))

    @pl.when(asks)
    def _():
        with jax.named_scope("fhello"):
            pl.semaphore_wait(far_hello, 1)

    @pl.when(sends_far)
    def _():
        each(TILES, lambda t: far_copy(0, t, b - 2 * s).start())

    @pl.when(no_far)
    def _():
        each(TILES, lambda t: far_copy(1, t, b + 2 * s).start())

    def scores(left, right):
        return lax.dot_general(
            left, right, (((1,), (1,)), ((), ())), preferred_element_type=jnp.float32
        )

    def own_unit(u):
        left = unit[tile_rows(u, UNIT), :]
        for n in range(UNITS):
            span = slice(n * UNIT, n * UNIT + UNIT)
            block = scores(left, unit[span, :])
            at = lax.broadcasted_iota(jnp.int32, (UNIT, UNIT), 0) + u * UNIT
            to = lax.broadcasted_iota(jnp.int32, (UNIT, UNIT), 1) + n * UNIT
            block = jnp.where(at == to, -jnp.inf, block)
            for q in range(UNIT // TILE):
                out_ref[pl.ds(16 + 2 * u + q, 1), span] = (
                    jnp.max(block[q * TILE : q * TILE + TILE, :], axis=0, keepdims=True) * scale
                )

    def pair_unit(keys_ref, rows_ref, u, by_row, row_base, by_key, key_base, parts=UNITS, first=0):
        left = keys_ref[tile_rows(u, UNIT), :]
        for n in range(first, parts):
            span = slice(n * UNIT, n * UNIT + UNIT)
            block = scores(left, rows_ref[span, :])
            for q in range(UNIT // TILE):
                part = block[q * TILE : q * TILE + TILE, :]
                by_row[pl.ds(row_base + 2 * u + q, 1), span] = (
                    jnp.max(part, axis=0, keepdims=True) * scale
                )
                columns = pl.ds(pl.multiple_of(u * UNIT + q * TILE, TILE), TILE)
                for h in range(UNIT // TILE):
                    turned = jnp.transpose(part[:, h * TILE : h * TILE + TILE])
                    by_key[pl.ds(key_base + 2 * n + h, 1), columns] = (
                        jnp.max(turned, axis=0, keepdims=True) * scale
                    )

    def slot(offset):
        return pl.multiple_of((offset + 2) * TILES, TILES)

    def take(landing, ref, sems, u):
        rows = tile_rows(u, UNIT)
        pltpu.make_async_copy(raw.at[rows], landing.at[rows], sems.at[u]).wait()
        normalise(landing, ref, u)

    def message(k, block, offset):
        return remote(
            back.at[pl.ds(k * TILES, TILES)],
            out_ref.at[pl.ds(slot(offset), TILES)],
            back_send.at[k],
            back_sem.at[offset + 2],
            block,
        )

    def far_unit(u):
        with jax.named_scope("farw"):
            take(far_in, far, far_sem, u)
        with jax.named_scope("farc"):
            pair_unit(far, unit, u, out_ref, slot(2 * s), back, 0)

    def near_take(u):
        with jax.named_scope("nearw"):
            take(near_in, near, near_sem, u)

    def near_score(u):
        with jax.named_scope("nearc"):
            pair_unit(near, unit, u, out_ref, slot(s), back, TILES)

    def near_unit(u):
        near_take(u)
        near_score(u)

    def near_far_unit(u):
        with jax.named_scope("nfc"):
            pair_unit(near, far, u, back, 2 * TILES, back, 3 * TILES)

    def extra_take(u):
        with jax.named_scope("xw"):
            take(extra_in, extra, extra_sem, u)

    def far_near_unit(u):
        with jax.named_scope("fnc"):
            pair_unit(far, near, u, back, 3 * TILES, back, 2 * TILES, 2)

    def extra_score(u):
        with jax.named_scope("xuc"):
            pair_unit(extra, unit, u, out_ref, slot(1), back, 4 * TILES)

    def extra_unit(u):
        extra_take(u)
        extra_score(u)

    def extra_near_unit(u, parts=UNITS - 1):
        with jax.named_scope("xnc"):
            pair_unit(extra, near, u, back, 5 * TILES, back, 6 * TILES, parts)

    def extra_near_span(u, first, parts):
        with jax.named_scope("xns"):
            pair_unit(extra, near, u, back, 5 * TILES, back, 6 * TILES, parts, first)

    def last_near_extra(parts=UNITS):
        with jax.named_scope("nxc"):
            pair_unit(near, extra, UNITS - 1, back, 6 * TILES, back, 5 * TILES, parts)

    def seam_forward(t):
        rows = tile_rows(t, PIECE)
        with jax.named_scope("passw"):
            pltpu.make_async_copy(raw.at[rows], pass_on.at[rows], pass_sem.at[t]).wait()
        seam_pass(t, pass_to).start()

    @pl.when(passes)
    def _():
        @pl.when(pass_o)
        def _():
            with jax.named_scope("hello"):
                pl.semaphore_wait(hello, 1)

        each(LEAD, seam_forward)

    def forward(i):
        @pl.when(both(passes, i < STEPS))
        def _():
            seam_forward(LEAD + 2 * i)
            seam_forward(LEAD + 2 * i + 1)

        @pl.when(i < around)
        def _():
            rows = tile_rows(i, PIECE)
            with jax.named_scope("ringw"):
                pltpu.make_async_copy(raw.at[rows], ring.at[rows], ring_sem.at[i]).wait()

            @pl.when(even)
            def _():
                leg_two(i).start()

            @pl.when(odd)
            def _():
                leg_three(i).start()

        @pl.when(both(slow, odd, i == SEAM_AROUND - 1))
        def _():
            each(direct, lambda j: straight(j).start())

        @pl.when(i < UNITS)
        def _():
            with jax.named_scope("own"):
                own_unit(i)

    each(jnp.where(slow, SEAM_AROUND, STEPS), forward)

    plain = both(even, jnp.logical_not(cross_e))

    def arrive(k):
        @pl.when(both(even, step_in, k == 2))
        def _():
            near_unit(1)

        @pl.when(both(even, step_in, k == 3))
        def _():
            each(3, far_near_unit)
            near_unit(2)

        @pl.when(has_far)
        def _():
            far_unit(k)

        @pl.when(both(even, step_in, k == 3))
        def _():
            far_near_unit(3)

        @pl.when(
            both(
                plain,
                jnp.logical_not(slow),
                jnp.logical_or(k == 1, both(k == 2, jnp.logical_not(step_in))),
            )
        )
        def _():
            near_unit(k - 1)

    each(UNITS, arrive)

    @pl.when(has_far)
    def _():
        message(0, b + 2 * s, -2 * s).start()

    @pl.when(plain)
    def _():
        def rest(k):
            @pl.when(both(cross_o, k == 2))
            def _():
                each(2, extra_take)
                each(2, lambda u: extra_near_unit(u, 2))

            @pl.when(jnp.logical_or(both(k == 2, jnp.logical_not(step_in)), both(slow, k < 2)))
            def _():
                near_unit(k)

            @pl.when(both(cross_o, k == 2))
            def _():
                each(2, lambda u: extra_near_span(u, 2, UNITS - 1))

            @pl.when(both(cross_o, k == 3))
            def _():
                extra_take(2)
                extra_near_unit(2)

            @pl.when(k == 3)
            def _():
                near_take(3)

            @pl.when(both(has_far, jnp.logical_or(k >= 2, jnp.logical_not(step_in))))
            def _():
                near_far_unit(k)

        each(UNITS, rest)

        @pl.when(has_far)
        def _():
            message(2, b + 2 * s, -s).start()
            message(3, mate, s).start()

        near_score(3)
        message(1, mate, -s).start()

        @pl.when(cross_o)
        def _():
            last_near_extra(UNITS - 1)
            extra_take(3)
            extra_near_unit(3, UNITS)
            message(5, mate, -2).start()

    @pl.when(cross_e)
    def _():
        def all_three(u):
            near_unit(u)
            near_far_unit(u)
            extra_unit(u)

        each(UNITS - 1, all_three)
        each(UNITS - 1, extra_near_unit)
        near_take(3)
        last_near_extra(UNITS - 1)
        extra_take(3)
        extra_near_unit(3, UNITS)
        message(6, over, -2).start()
        message(5, mate, 2).start()
        extra_score(3)
        message(4, over, -1).start()
        near_far_unit(3)
        message(2, b + 2 * s, -s).start()
        message(3, mate, s).start()
        near_score(3)
        message(1, mate, -s).start()

    @pl.when(cross_o)
    def _():
        pl.semaphore_wait(hello, 1)
        message(6, over, 2).start()

    def landed(offset):
        pltpu.make_async_copy(
            back.at[pl.ds(0, TILES)],
            out_ref.at[pl.ds(slot(offset), TILES)],
            back_sem.at[offset + 2],
        ).wait()

    with jax.named_scope("landed"):
        landed(-2 * s)

        @pl.when(jnp.logical_not(cross_e))
        def _():
            landed(-s)

        @pl.when(odd)
        def _():
            landed(s)

        @pl.when(no_far)
        def _():
            landed(2 * s)

    with jax.named_scope("settle"):
        def left(condition, sem, rows=ROWS):
            @pl.when(condition)
            def _():
                part = pl.ds(0, rows)
                pltpu.make_async_copy(raw.at[part], raw.at[part], sem).wait()

        usual = jnp.logical_not(last_e)
        left(both(usual, low), ring_send, AROUND * PIECE)
        left(both(usual, high), ring_send, (AROUND + 1) * PIECE)
        left(slow, ring_send, SEAM_AROUND * PIECE)
        left(odd, near_send)
        left(sends_far, far_send.at[0])
        left(no_far, far_send.at[1])
        left(cross, extra_send)
        left(passes, pass_send)

        @pl.when(has_far)
        def _():
            message(0, b + 2 * s, -2 * s).wait_send()

        @pl.when(even)
        def _():
            message(1, mate, -s).wait_send()

            @pl.when(has_far)
            def _():
                message(2, b + 2 * s, -s).wait_send()
                message(3, mate, s).wait_send()

        @pl.when(cross_e)
        def _():
            message(4, over, -1).wait_send()

        @pl.when(cross)
        def _():
            message(5, mate, 2 * s).wait_send()
            message(6, over, 2 * s).wait_send()


def body(embeddings):
    rows, width = embeddings.shape
    block = pltpu.VMEM((rows, width), jnp.bfloat16)
    dma = pltpu.SemaphoreType.DMA
    tiles_t = pl.pallas_call(
        kernel,
        name="cycle_tile_max",
        out_shape=jax.ShapeDtypeStruct((5 * TILES, rows), jnp.float32),
        in_specs=[pl.BlockSpec(memory_space=pltpu.HBM)],
        out_specs=pl.BlockSpec(memory_space=pltpu.VMEM),
        scratch_shapes=[
            block,
            block,
            block,
            block,
            block,
            block,
            block,
            block,
            block,
            pltpu.VMEM((SEAM_AROUND * PIECE, width), jnp.bfloat16),
            pltpu.VMEM((7 * TILES, rows), jnp.float32),
            dma,
            dma,
            dma((UNITS,)),
            dma,
            dma((SEAM_AROUND,)),
            dma((2,)),
            dma((UNITS,)),
            dma,
            dma((UNITS,)),
            dma((PIECES,)),
            dma,
            dma((7,)),
            dma((5,)),
            pltpu.SemaphoreType.REGULAR,
            pltpu.SemaphoreType.REGULAR,
        ],
        compiler_params=pltpu.CompilerParams(
            collective_id=0, has_side_effects=True, vmem_limit_bytes=52 * 2**20
        ),
        cost_estimate=pl.CostEstimate(
            flops=8 * 1024**3, bytes_accessed=4 * 2**20, transcendentals=0
        ),
    )(embeddings)
    return jnp.transpose(tiles_t)


def solution(mesh):
    return jax.shard_map(
        body,
        mesh=mesh,
        in_specs=(P(("blk", "grp"), None),),
        out_specs=P(("blk", "grp"), None),
        check_vma=False,
    )
```
